128 devices in a mesh: irrep: 4 (over z), occ: 4 (over y), vir: 8 (over x, core).
Axes of the slice: x: 4, y: 4, z: 4, core: 2. Of those that a mesh axis runs over, the one named last changes fastest.
Arguments:
- amplitudes: bfloat16 [8, 320, 12288], P('irrep', None, ('occ', 'vir')), may hold values from -6 to 6
- ladder_ints: bfloat16 [8, 12288, 12288], P('irrep', ('occ', 'vir')), may hold values from -0.109375 to 0.109375
- hole_ints: bfloat16 [8, 320, 320], P('irrep'), may hold values from -0.3125 to 0.3125
- occ_energy: float32 [8, 320], P('irrep'), may hold values from -3 to -0.5
- vir_energy: float32 [8, 12288], P('irrep', ('occ', 'vir')), may hold values from 0.5 to 3
- occ_pairs: int32 [8], replicated, may hold values from 160 to 320, as said below
- vir_pairs: int32 [8], replicated, may hold values from 6144 to 12288, as said below
Outputs:
- updated: bfloat16 [8, 320, 12288], P('irrep', None, ('occ', 'vir'))
- residual_norm: float32 [8], P('irrep')
The draws below stay inside these ranges and needn't reach their ends.
Inputs may be any that keep to these rules, and one draw needn't show every extreme that they name: `occ_pairs`: some block has exactly 320 live occupied pairs in every draw. `vir_pairs`: some block has exactly 12288 live virtual pairs in every draw.
All inputs are finite; a program needn't handle non-finite values.
Results may differ from the reference program's by a relative error of at most 0.001.
Values may be sent and summed in bfloat16 or wider, within the bound.
A program may use at most 128 MiB of HBM per device.

```python
import jax
import jax.numpy as jnp

NB = 8
OP = 320
VP = 12288


def draw_occ_pairs(key, part):
    first_key, second_key = jax.random.split(jax.random.fold_in(key, 11))
    values = jax.random.randint(first_key, (NB,), OP // 2, OP + 1)
    chosen = jax.random.randint(second_key, (), 0, NB)
    return jnp.where(jnp.arange(NB) == chosen, OP, values).astype(jnp.int32)


def draw_vir_pairs(key, part):
    first_key, second_key = jax.random.split(jax.random.fold_in(key, 23))
    values = jax.random.randint(first_key, (NB,), VP // 2, VP + 1)
    chosen = jax.random.randint(second_key, (), 0, NB)
    return jnp.where(jnp.arange(NB) == chosen, VP, values).astype(jnp.int32)


def with_spikes(drawn, stream_key, source, target, shards_of, factor):
    def block_of(dim):
        return (jnp.arange(drawn.shape[dim]) // (drawn.shape[dim] // shards_of)).reshape((-1,) + (1,) * (drawn.ndim - 1 - dim))

    near = jax.random.permutation(stream_key, shards_of)[block_of(target)]
    second = (block_of(target) + shards_of // 2) % shards_of
    return jnp.where((block_of(source) == near) | (block_of(source) == second), factor * drawn, drawn)


def shard_levels(stream_key, shape, pieces, low, largest):
    def one(position, blocks):
        steps = jax.random.uniform(jax.random.fold_in(jax.random.fold_in(stream_key, 6), position), (blocks,), jnp.float32, low / len(pieces), largest / len(pieces))
        return jnp.repeat(jnp.exp(steps), shape[position] // blocks).reshape((-1,) + (1,) * (len(shape) - position - 1))

    gain = one(*pieces[0])
    for cut in pieces[1:]:
        gain = gain * one(*cut)
    return gain


def centred(stream_key, dims, scale, bound, cuts=(), kind=jnp.bfloat16):
    gain = shard_levels(stream_key, dims, cuts, -0.22, 0.18) if cuts else 1.0
    result = jax.random.normal(stream_key, dims, jnp.float32) * scale * gain
    return jnp.minimum(jnp.maximum(result, -bound), bound).astype(kind)


def heavy_noise(own_key, shape, deviation, bound, shards, heavy, kind=jnp.bfloat16):
    entries = deviation * jax.random.normal(own_key, shape, jnp.float32)
    if shards:
        entries = entries * shard_levels(own_key, shape, shards, -0.22, 0.18)
    return jnp.clip(with_spikes(entries, jax.random.fold_in(own_key, 3), *heavy), -bound, bound).astype(kind)


def setup_inputs(seed: int = 0) -> dict:
    splits = jax.random.split(jax.random.key(seed), 8)
    amplitudes = centred(splits[0], (NB, OP, VP), 1.0, 6.0, ((0, 4), (2, 32)))
    ladder_ints = heavy_noise(splits[1], (NB, VP, VP), VP ** -0.5, 0.109375, ((0, 4), (1, 32)), (1, 2, 32, 2.75))
    hole_ints = centred(splits[2], (NB, OP, OP), OP ** -0.5, 0.3125, ((0, 4),))
    occ_energy = jnp.clip(-3.0 + 2.5 * jax.random.uniform(splits[3], (NB, OP), jnp.float32) ** shard_levels(splits[3], (NB, OP), ((0, 4),), -0.2, 0.2), -3.0, -0.5)
    vir_energy = jnp.clip(0.5 + 2.5 * jax.random.uniform(splits[4], (NB, VP), jnp.float32) ** shard_levels(splits[4], (NB, VP), ((0, 4), (1, 32)), -0.2, 0.2), 0.5, 3.0)
    occ_pairs = draw_occ_pairs(jax.random.fold_in(splits[7], 71), 0)
    vir_pairs = draw_vir_pairs(jax.random.fold_in(splits[7], 71), 0)
    return dict(amplitudes=amplitudes, ladder_ints=ladder_ints, hole_ints=hole_ints, occ_energy=occ_energy, vir_energy=vir_energy, occ_pairs=occ_pairs, vir_pairs=vir_pairs)


LEVEL_SHIFT = 0.5
EPSILON = 1e-06

def reference(amplitudes, ladder_ints, hole_ints, occ_energy, vir_energy, occ_pairs, vir_pairs):
    row_index = jnp.arange(OP, dtype=jnp.int32)
    col_index = jnp.arange(VP, dtype=jnp.int32)
    results = []
    norms = []
    for block in range(NB):
        keep_mask = (row_index[:, None] < occ_pairs[block]) & (col_index[None, :] < vir_pairs[block])
        masked = jnp.where(keep_mask, amplitudes[block], jnp.zeros((), amplitudes.dtype))
        ladder_term = jnp.dot(masked, ladder_ints[block], preferred_element_type=jnp.float32)
        hole_term = jnp.dot(hole_ints[block], masked, preferred_element_type=jnp.float32)
        wide = masked.astype(jnp.float32)
        denominator = vir_energy[block][None, :] - occ_energy[block][:, None]
        residual = jnp.where(keep_mask, ladder_term + hole_term + denominator * wide, jnp.zeros((), jnp.float32))
        updated = wide - residual / (denominator + LEVEL_SHIFT)
        pair_count = (occ_pairs[block] * vir_pairs[block]).astype(jnp.float32)
        results.append(updated.astype(jnp.bfloat16))
        norms.append(jnp.sqrt(jnp.sum(residual * residual) / pair_count + EPSILON))
    return (jnp.stack(results), jnp.stack(norms))
```

```python
import functools

import jax
import jax.numpy as jnp
from jax import lax
from jax.experimental import pallas as pl
from jax.experimental.pallas import tpu as pltpu
from jax.sharding import PartitionSpec as P

LEVEL_SHIFT = 0.5
EPSILON = 1e-06
MESH = pl.DeviceIdType.MESH
REL = (2, 1, 3, 0)
STEPS_PER_OCTAVE = 128.0
CODE_RANGE = 32000.0
TINY = 1e-33


def kernel(
    dims,
    occ_pairs,
    vir_pairs,
    amp,
    hole,
    occ_e,
    vir_e,
    lad,
    out,
    norm_out,
    amp_peer,
    amat,
    ladbuf,
    part,
    gain,
    msg_out,
    msg_in,
    two_out,
    two_in,
    sq_mine,
    sq_all,
    amp_s,
    amp_r,
    lad_l,
    lad_s,
    lad_r,
    one_s,
    one_r,
    two_s,
    two_r,
    sq_s,
    sq_r,
):
    nx, ny = dims
    rows, cols = amp.shape[1:]
    half = rows // 2
    lanes = cols // 128
    groups = half // 16
    z, y, v = lax.axis_index("irrep"), lax.axis_index("occ"), lax.axis_index("vir")
    x, c = v // 2, v % 2
    peer = {"vir": x * 2 + (1 - c)}
    size = {0: nx, 1: ny}

    def shifted(axis, by):
        if axis == 0:
            return {"vir": ((x + by) % nx) * 2 + c}
        return {"occ": (y + by) % ny}

    def columns(b, s, t, core):
        i, j = (x, y) if b == 0 else (y, x)
        to_i, to_j = (i + REL[t]) % 4, (j + REL[s]) % 4
        to_x, to_y = (to_i, to_j) if b == 0 else (to_j, to_i)
        return pl.ds(pl.multiple_of(((to_y * nx + to_x) * 2 + core) * cols, 128), cols)

    for s in range(4):
        for t in range(4):
            for b in range(2):
                pltpu.make_async_copy(
                    lad.at[b, :, columns(b, s, t, c)],
                    ladbuf.at[b, s, pl.ds(0, cols), pl.ds(t * cols, cols)],
                    lad_l.at[b, s, t // 2],
                ).start()

    barrier = pltpu.get_barrier_semaphore()
    others = [(dy, dv) for dy in range(ny) for dv in range(2 * nx) if dy or dv]
    for dy, dv in others:
        pl.semaphore_signal(
            barrier, inc=1, device_id={"occ": (y + dy) % ny, "vir": (v + dv) % (2 * nx)}, device_id_type=MESH
        )
    pl.semaphore_wait(barrier, len(others))

    amp_copy = pltpu.make_async_remote_copy(amp, amp_peer, amp_s, amp_r, device_id=peer, device_id_type=MESH)
    amp_copy.start()
    for s in range(4):
        for t in range(4):
            for b in range(2):
                pltpu.make_async_remote_copy(
                    lad.at[b, :, columns(b, s, t, 1 - c)],
                    ladbuf.at[b, s, pl.ds(cols, cols), pl.ds(t * cols, cols)],
                    lad_s.at[b, s],
                    lad_r.at[b, s, t // 2],
                    device_id=peer,
                    device_id_type=MESH,
                ).start()

    def keep(b, core):
        n_occ, n_vir = occ_pairs[z * 2 + b], vir_pairs[z * 2 + b]
        first = ((y * nx + x) * 2 + core) * cols
        row = lax.broadcasted_iota(jnp.int32, (rows, cols), 0)
        col = lax.broadcasted_iota(jnp.int32, (rows, cols), 1) + first
        return (row < n_occ) & (col < n_vir)

    def masked(values, b, core):
        return jnp.where(keep(b, core), values.astype(jnp.float32), 0.0)

    def energy_gap(b):
        occ_col = jnp.broadcast_to(occ_e[b : b + 1, :], (128, rows)).T
        return vir_e[b : b + 1, :] - jnp.concatenate([occ_col] * lanes, axis=1)

    for b in range(2):
        wide = masked(amp[b], b, c)
        narrow = wide.astype(jnp.bfloat16)
        amat[b, :, pl.ds(0, cols)] = narrow
        gain[b] = jnp.dot(hole[b], narrow, preferred_element_type=jnp.float32) + energy_gap(b) * wide
    amp_copy.wait_recv()
    for b in range(2):
        amat[b, :, pl.ds(cols, cols)] = masked(amp_peer[b], b, 1 - c).astype(jnp.bfloat16)

    def encode(read, message):
        biggest = None
        for k in range(lanes):
            here = jnp.max(jnp.abs(read(k)).reshape(groups, 16, 128), axis=0)
            biggest = here if biggest is None else jnp.maximum(biggest, here)
        code = jnp.ceil(jnp.log2(jnp.maximum(biggest, TINY)) * STEPS_PER_OCTAVE) + 1.0
        up = jnp.exp2(code * (-1.0 / STEPS_PER_OCTAVE)) * CODE_RANGE
        for k in range(lanes):
            steps = jnp.round(read(k).reshape(groups, 16, 128) * up[None])
            message[pl.ds(k * groups, groups)] = steps.astype(jnp.int32).astype(jnp.int16)
        message[lanes * groups] = code.astype(jnp.int32).astype(jnp.int16)

    def decoded(message):
        code = message[lanes * groups].astype(jnp.int32).astype(jnp.float32)
        down = jnp.exp2(code * (1.0 / STEPS_PER_OCTAVE)) * (1.0 / CODE_RANGE)

        def read(k):
            steps = message[pl.ds(k * groups, groups)].astype(jnp.int32).astype(jnp.float32)
            return (steps * down[None]).reshape(half, 128)

        return read

    def piece(b, s, t, h):
        def ref(k):
            return part.at[b, s, pl.ds(h * half, half), pl.ds(t * cols + k * 128, 128)]

        return ref

    def values(ref):
        return lambda k: ref(k)[...]

    def add_into(ref, messages):
        reads = [decoded(m) for m in messages]
        for k in range(lanes):
            total = ref(k)[...]
            for read in reads:
                total = total + read(k)
            ref(k)[...] = total

    def send_one(b, s, m):
        return pltpu.make_async_remote_copy(
            msg_out.at[b, s, m],
            msg_in.at[b, s, m],
            one_s.at[b, s, m],
            one_r.at[b, s, m],
            device_id=shifted(b, 1 - 2 * (m % 2)),
            device_id_type=MESH,
        )

    def send_two(b, m):
        return pltpu.make_async_remote_copy(
            two_out.at[b, m],
            two_in.at[b, m],
            two_s.at[b, m],
            two_r.at[b, m],
            device_id=shifted(1 - b, 1 - 2 * (m % 2)),
            device_id_type=MESH,
        )

    def stage_a(s):
        for u in range(2):
            for b in range(2):
                width = pl.ds(u * 2 * cols, 2 * cols)
                mine = ladbuf.at[b, s, pl.ds(0, cols), width]
                pltpu.make_async_copy(mine, mine, lad_l.at[b, s, u]).wait()
                theirs = ladbuf.at[b, s, pl.ds(cols, cols), width]
                pltpu.make_async_copy(theirs, theirs, lad_r.at[b, s, u]).wait()
                part[b, s, :, width] = jnp.dot(
                    amat[b], ladbuf[b, s, :, width], preferred_element_type=jnp.float32
                )
                if u == 0:
                    encode(values(piece(b, s, 0, 0)), msg_out.at[b, s, 0])
                    encode(values(piece(b, s, 0, 1)), msg_out.at[b, s, 1])
                    send_one(b, s, 0).start()
                    send_one(b, s, 1).start()
                    encode(values(piece(b, s, 1, 1)), msg_out.at[b, s, 2])
                    send_one(b, s, 2).start()
                else:
                    encode(values(piece(b, s, 2, 0)), msg_out.at[b, s, 3])
                    send_one(b, s, 3).start()

    def stage_b(s):
        for b in range(2):
            for m, t in ((0, 1), (1, 2)):
                send_one(b, s, m).wait_recv()
                add_into(piece(b, s, t, m), [msg_in.at[b, s, m]])
                encode(values(piece(b, s, t, m)), msg_out.at[b, s, 4 + m])
                send_one(b, s, 4 + m).start()

    def stage_c(s):
        for b in range(2):
            for h, pair in enumerate(((4, 3), (2, 5))):
                for m in pair:
                    send_one(b, s, m).wait_recv()
                add_into(piece(b, s, 3, h), [msg_in.at[b, s, m] for m in pair])

    def two_first(s):
        for b in range(2):
            for m, (at, h) in enumerate(((0, 0), (0, 1), (1, 1), (2, 0))):
                if at == s:
                    encode(values(piece(b, s, 3, h)), two_out.at[b, m])
                    send_two(b, m).start()

    def two_second():
        for b in range(2):
            for m, s in ((0, 1), (1, 2)):
                send_two(b, m).wait_recv()
                add_into(piece(b, s, 3, m), [two_in.at[b, m]])
                encode(values(piece(b, s, 3, m)), two_out.at[b, 4 + m])
                send_two(b, 4 + m).start()

    def loop(t, carry):
        @pl.when(t < 4)
        def _():
            stage_a(t)

        @pl.when((t > 0) & (t < 5))
        def _():
            stage_b(t - 1)

        @pl.when(t > 1)
        def _():
            stage_c(t - 2)

        for s in range(3):

            @pl.when(t == s + 2)
            def _():
                two_first(s)

        @pl.when(t == 4)
        def _():
            two_second()

        return carry

    lax.fori_loop(0, 6, loop, 0)

    for b in range(2):
        for h, pair in enumerate(((4, 3), (2, 5))):
            for m in pair:
                send_two(b, m).wait_recv()
            add_into(piece(b, 3, 3, h), [two_in.at[b, m] for m in pair])
        wide = amat[b, :, pl.ds(0, cols)].astype(jnp.float32)
        ladder = part[b, 3, :, pl.ds(3 * cols, cols)]
        residual = jnp.where(keep(b, c), ladder + gain[b], 0.0)
        out[b] = (wide - residual / (energy_gap(b) + LEVEL_SHIFT)).astype(jnp.bfloat16)
        lane_sums = jnp.sum(residual * residual, axis=0, keepdims=True)
        total = lane_sums[:, :128]
        for k in range(1, lanes):
            total = total + lane_sums[:, k * 128 : (k + 1) * 128]
        sq_mine[pl.ds(b, 1), :] = total

    def send_sq(dy, dv, slot):
        return pltpu.make_async_remote_copy(
            sq_mine,
            sq_all.at[slot],
            sq_s,
            sq_r,
            device_id={"occ": (y + dy) % ny, "vir": (v + dv) % (2 * nx)},
            device_id_type=MESH,
        )

    for slot, (dy, dv) in enumerate(others):
        send_sq(dy, dv, slot).start()
    pltpu.make_async_copy(sq_all, sq_all, sq_r).wait()
    total = jnp.sum(sq_all[...], axis=0) + sq_mine[...]
    total = jnp.broadcast_to(jnp.sum(total, axis=1, keepdims=True), (2, 128))
    counts = [(occ_pairs[z * 2 + b] * vir_pairs[z * 2 + b]).astype(jnp.float32) for b in range(2)]
    block = lax.broadcasted_iota(jnp.int32, (2, 128), 0)
    norm_out[...] = jnp.sqrt(total / jnp.where(block == 0, counts[0], counts[1]) + EPSILON)

    pltpu.make_async_copy(sq_all, sq_all, sq_s).wait()
    amp_copy.wait_send()

    def drain(s, carry):
        for b in range(2):
            theirs = ladbuf.at[b, s, pl.ds(cols, cols), :]
            pltpu.make_async_copy(theirs, theirs, lad_s.at[b, s]).wait()
            for m in range(6):
                send_one(b, s, m).wait_send()
        return carry

    lax.fori_loop(0, 4, drain, 0)
    for b in range(2):
        for m in range(6):
            send_two(b, m).wait_send()


def body(amplitudes, ladder_ints, hole_ints, occ_energy, vir_energy, occ_pairs, vir_pairs):
    blocks, rows, cols = amplitudes.shape
    ny, nv = lax.axis_size("occ"), lax.axis_size("vir")
    nx = nv // 2
    tiles = (rows // 32) * (cols // 128) + 1
    smem, vmem = pl.BlockSpec(memory_space=pltpu.SMEM), pl.BlockSpec(memory_space=pltpu.VMEM)
    dma = pltpu.SemaphoreType.DMA
    updated, norm = pl.pallas_call(
        functools.partial(kernel, (nx, ny)),
        out_shape=(
            jax.ShapeDtypeStruct((blocks, rows, cols), jnp.bfloat16),
            jax.ShapeDtypeStruct((2, 128), jnp.float32),
        ),
        in_specs=[smem, smem, vmem, vmem, vmem, vmem, pl.BlockSpec(memory_space=pl.ANY)],
        out_specs=(vmem, vmem),
        scratch_shapes=[
            pltpu.VMEM((2, rows, cols), jnp.bfloat16),
            pltpu.VMEM((2, rows, 2 * cols), jnp.bfloat16),
            pltpu.VMEM((2, 4, 2 * cols, 4 * cols), jnp.bfloat16),
            pltpu.VMEM((2, 4, rows, 4 * cols), jnp.float32),
            pltpu.VMEM((2, rows, cols), jnp.float32),
            pltpu.VMEM((2, 4, 6, tiles, 16, 128), jnp.int16),
            pltpu.VMEM((2, 4, 6, tiles, 16, 128), jnp.int16),
            pltpu.VMEM((2, 6, tiles, 16, 128), jnp.int16),
            pltpu.VMEM((2, 6, tiles, 16, 128), jnp.int16),
            pltpu.VMEM((2, 128), jnp.float32),
            pltpu.VMEM((ny * nv - 1, 2, 128), jnp.float32),
            dma,
            dma,
            dma((2, 4, 2)),
            dma((2, 4)),
            dma((2, 4, 2)),
            dma((2, 4, 6)),
            dma((2, 4, 6)),
            dma((2, 6)),
            dma((2, 6)),
            dma,
            dma,
        ],
        compiler_params=pltpu.CompilerParams(
            collective_id=0, has_side_effects=True, vmem_limit_bytes=66_000_000
        ),
    )(occ_pairs, vir_pairs, amplitudes, hole_ints, occ_energy, vir_energy, ladder_ints)
    return updated, norm[:, 0]


def solution(mesh):
    in_specs = (
        P("irrep", None, ("occ", "vir")),
        P("irrep", ("occ", "vir"), None),
        P("irrep", None, None),
        P("irrep", None),
        P("irrep", ("occ", "vir")),
        P(),
        P(),
    )
    out_specs = (P("irrep", None, ("occ", "vir")), P("irrep"))
    return jax.shard_map(body, mesh=mesh, in_specs=in_specs, out_specs=out_specs, check_vma=False)
```

```python
import functools

import jax
import jax.numpy as jnp
from jax import lax
from jax.experimental import pallas as pl
from jax.experimental.pallas import tpu as pltpu
from jax.sharding import PartitionSpec as P

LEVEL_SHIFT = 0.5
EPSILON = 1e-06
MESH = pl.DeviceIdType.MESH
SPLIT = (slice(0, 1), slice(1, 4))
ORDER = ((0, 0), (1, 0), (0, 1), (2, 0), (1, 1), (3, 0), (2, 1), (3, 1))
REL = (2, 1, 3, 0)
STEPS_PER_OCTAVE = 128.0
CODE_RANGE = 32000.0
TINY = 1e-33


def kernel(
    dims,
    occ_pairs_hbm,
    vir_pairs_hbm,
    amp_hbm,
    hole_hbm,
    occ_e_hbm,
    vir_e_hbm,
    lad,
    out,
    norm_out,
    occ_pairs,
    vir_pairs,
    amp,
    hole,
    occ_e,
    vir_e,
    amp_peer,
    first,
    amat,
    ladbuf,
    part,
    gain,
    msg_out,
    msg_in,
    two_out,
    two_in,
    sq_mine,
    sq_all,
    load_s,
    first_s,
    amp_s,
    amp_r,
    lad_s,
    lad_r,
    one_s,
    one_r,
    two_s,
    two_r,
    sq_s,
    sq_r,
):
    nx, ny = dims
    rows, cols = amp.shape[1:]
    half = rows // 2
    lanes = cols // 128
    groups = half // 8
    data = lanes * groups
    z, y, v = lax.axis_index("irrep"), lax.axis_index("occ"), lax.axis_index("vir")
    x, c = v // 2, v % 2
    peer = {"vir": x * 2 + (1 - c)}
    size = {0: nx, 1: ny}

    def shifted(axis, by):
        if axis == 0:
            return {"vir": ((x + by) % nx) * 2 + c}
        return {"occ": (y + by) % ny}

    def columns(b, s, t, core):
        i, j = (x, y) if b == 0 else (y, x)
        to_i, to_j = (i + REL[t]) % 4, (j + REL[s]) % 4
        to_x, to_y = (to_i, to_j) if b == 0 else (to_j, to_i)
        return pl.ds(pl.multiple_of(((to_y * nx + to_x) * 2 + core) * cols, 128), cols)

    barrier = pltpu.get_barrier_semaphore()
    neighbours = [peer] + [shifted(axis, by) for axis in (0, 1) for by in (1, -1)]
    for device in neighbours:
        pl.semaphore_signal(barrier, inc=1, device_id=device, device_id_type=MESH)

    def load(n):
        src, dst = (
            (amp_hbm, amp),
            (occ_pairs_hbm, occ_pairs),
            (vir_pairs_hbm, vir_pairs),
            (occ_e_hbm, occ_e),
            (vir_e_hbm, vir_e),
            (hole_hbm, hole),
        )[n]
        return pltpu.make_async_copy(src, dst, load_s.at[n])

    def load_first(b):
        return pltpu.make_async_copy(lad.at[b, :, columns(b, 0, 0, 1 - c)], first.at[b], first_s.at[b])

    def load_ladder(g):
        s, u = ORDER[g]
        for b in range(2):
            for t in range(4)[SPLIT[u]]:
                pltpu.make_async_copy(
                    lad.at[b, :, columns(b, s, t, c)],
                    ladbuf.at[b, s, pl.ds(0, cols), pl.ds(t * cols, cols)],
                    lad_r.at[b, s, u],
                ).start()

    def swap_ladder(g):
        s, u = ORDER[g]
        for b in range(2):
            if g == 0:
                swap_amp(b).start()
            for t in range(4)[SPLIT[u]]:
                pltpu.make_async_remote_copy(
                    first.at[b] if g == 0 else lad.at[b, :, columns(b, s, t, 1 - c)],
                    ladbuf.at[b, s, pl.ds(cols, cols), pl.ds(t * cols, cols)],
                    lad_s.at[s],
                    lad_r.at[b, s, u],
                    device_id=peer,
                    device_id_type=MESH,
                ).start()

    def swap_amp(b):
        return pltpu.make_async_remote_copy(
            amp.at[b], amp_peer.at[b], amp_s, amp_r.at[b], device_id=peer, device_id_type=MESH
        )

    load(0).start()
    for b in range(2):
        load_first(b).start()
    for n in (1, 2):
        load(n).start()
    load_ladder(0)
    pl.semaphore_wait(barrier, len(neighbours))
    load(0).wait()
    for b in range(2):
        load_first(b).wait()
    swap_ladder(0)
    load_ladder(1)
    swap_ladder(1)
    load_ladder(2)
    for n in (3, 4, 5):
        load(n).start()
    for n in (1, 2):
        load(n).wait()

    def keep(b, core):
        n_occ, n_vir = occ_pairs[z * 2 + b], vir_pairs[z * 2 + b]
        first = ((y * nx + x) * 2 + core) * cols
        row = lax.broadcasted_iota(jnp.int32, (rows, cols), 0)
        col = lax.broadcasted_iota(jnp.int32, (rows, cols), 1) + first
        return (row < n_occ) & (col < n_vir)

    def masked(values, b, core):
        return jnp.where(keep(b, core), values.astype(jnp.float32), 0.0)

    def energy_gap(b):
        occ_col = jnp.broadcast_to(occ_e[b : b + 1, :], (128, rows)).T
        return vir_e[b : b + 1, :] - jnp.concatenate([occ_col] * lanes, axis=1)

    def amplitudes(b):
        amat[b, :, pl.ds(0, cols)] = masked(amp[b], b, c).astype(jnp.bfloat16)
        swap_amp(b).wait_recv()
        amat[b, :, pl.ds(cols, cols)] = masked(amp_peer[b], b, 1 - c).astype(jnp.bfloat16)

    def local_terms(b):
        narrow = amat[b, :, pl.ds(0, cols)]
        hole_term = jnp.dot(hole[b], narrow, preferred_element_type=jnp.float32)
        gain[b] = hole_term + energy_gap(b) * narrow.astype(jnp.float32)

    def encode(ref, message):
        biggest = None
        for k in range(lanes):
            here = jnp.max(jnp.abs(ref(k)[...]).reshape(groups, 8, 128), axis=0)
            biggest = here if biggest is None else jnp.maximum(biggest, here)
        code = jnp.ceil(jnp.log2(jnp.maximum(biggest, TINY)) * STEPS_PER_OCTAVE) + 1.0
        up = jnp.exp2(code * (-1.0 / STEPS_PER_OCTAVE)) * CODE_RANGE
        for k in range(lanes):
            steps = jnp.round(ref(k)[...].reshape(groups, 8, 128) * up[None])
            message[pl.ds(k * groups, groups)] = steps.astype(jnp.int32).astype(jnp.int16)
        message[data] = code.astype(jnp.int32).astype(jnp.int16)

    def decoded(message):
        code = message[data].astype(jnp.int32).astype(jnp.float32)
        down = jnp.exp2(code * (1.0 / STEPS_PER_OCTAVE)) * (1.0 / CODE_RANGE)

        def read(k):
            steps = message[pl.ds(k * groups, groups)].astype(jnp.int32).astype(jnp.float32)
            return (steps * down[None]).reshape(half, 128)

        return read

    def piece(b, s, t, h):
        def ref(k):
            return part.at[b, s, pl.ds(h * half, half), pl.ds(t * cols + k * 128, 128)]

        return ref

    def add_into(ref, messages):
        reads = [decoded(m) for m in messages]
        for k in range(lanes):
            total = ref(k)[...]
            for read in reads:
                total = total + read(k)
            ref(k)[...] = total

    def send_one(b, s, m):
        return pltpu.make_async_remote_copy(
            msg_out.at[b, s, m],
            msg_in.at[b, s, m],
            one_s.at[s],
            one_r.at[b, s, min(m, 2)],
            device_id=shifted(b, 1 - 2 * (m % 2)),
            device_id_type=MESH,
        )

    def send_two(b, m):
        return pltpu.make_async_remote_copy(
            two_out.at[b, m],
            two_in.at[b, m],
            two_s,
            two_r.at[b, min(m, 2)],
            device_id=shifted(1 - b, 1 - 2 * (m % 2)),
            device_id_type=MESH,
        )

    def products(b, s, u):
        ts = range(4)[SPLIT[u]]
        width = pl.ds(ts[0] * cols, len(ts) * cols)
        both = ladbuf.at[b, s, :, width]
        pltpu.make_async_copy(both, both, lad_r.at[b, s, u]).wait()
        part[b, s, :, width] = jnp.dot(amat[b], ladbuf[b, s, :, width], preferred_element_type=jnp.float32)

    def emit(b, s, u):
        for d in range(2):
            t, h = (0, d) if u == 0 else (1 + d, 1 - d)
            encode(piece(b, s, t, h), msg_out.at[b, s, 2 * u + d])
            send_one(b, s, 2 * u + d).start()

    def stage_a(s, u):
        for b in range(2):
            if s == 0 and u == 0:
                amplitudes(b)
            products(b, s, u)
            emit(b, s, u)

    def stage_b(s):
        for b in range(2):
            for d in range(2):
                send_one(b, s, d).wait_recv()
                add_into(piece(b, s, 1 + d, d), [msg_in.at[b, s, d]])
                encode(piece(b, s, 1 + d, d), msg_out.at[b, s, 4 + d])
                send_one(b, s, 4 + d).start()

    def stage_c(s):
        for b in range(2):
            rest = msg_in.at[b, s, pl.ds(2, 4)]
            pltpu.make_async_copy(rest, rest, one_r.at[b, s, 2]).wait()
            for d in range(2):
                add_into(piece(b, s, 3, d), [msg_in.at[b, s, m] for m in (4 + d, 3 - d)])

    def two_first(m):
        at, h = ((0, 0), (0, 1), (1, 1), (2, 0))[m]
        for b in range(2):
            encode(piece(b, at, 3, h), two_out.at[b, m])
            send_two(b, m).start()

    def two_second(m):
        for b in range(2):
            send_two(b, m).wait_recv()
            add_into(piece(b, 1 + m, 3, m), [two_in.at[b, m]])
            encode(piece(b, 1 + m, 3, m), two_out.at[b, 4 + m])
            send_two(b, 4 + m).start()

    stage_a(0, 0)
    swap_ladder(2)
    load_ladder(3)
    stage_a(1, 0)
    stage_a(0, 1)
    swap_ladder(3)
    load_ladder(4)
    stage_b(0)
    swap_ladder(4)
    load_ladder(5)
    stage_a(2, 0)
    stage_a(1, 1)
    swap_ladder(5)
    load_ladder(6)
    swap_ladder(6)
    load_ladder(7)
    stage_b(1)
    stage_c(0)
    two_first(0)
    two_first(1)
    swap_ladder(7)
    stage_a(3, 0)
    stage_a(2, 1)
    stage_b(2)
    stage_c(1)
    two_first(2)
    for n in (3, 4, 5):
        load(n).wait()
    for b in range(2):
        products(b, 3, 1)
        local_terms(b)
    stage_b(3)
    two_second(0)
    for b in range(2):
        emit(b, 3, 1)
    stage_c(2)
    two_first(3)
    two_second(1)
    stage_c(3)

    for b in range(2):
        rest = two_in.at[b, pl.ds(2, 4)]
        pltpu.make_async_copy(rest, rest, two_r.at[b, 2]).wait()
        for h, pair in enumerate(((4, 3), (2, 5))):
            add_into(piece(b, 3, 3, h), [two_in.at[b, m] for m in pair])
        ladder = part[b, 3, :, pl.ds(3 * cols, cols)]
        residual = jnp.where(keep(b, c), ladder + gain[b], 0.0)
        gain[b] = residual
        lane_sums = jnp.sum(residual * residual, axis=0, keepdims=True)
        total = lane_sums[:, :128]
        for k in range(1, lanes):
            total = total + lane_sums[:, k * 128 : (k + 1) * 128]
        sq_mine[pl.ds(b, 1), :] = total

    others = [(dy, dv) for dy in range(ny) for dv in range(2 * nx) if dy or dv]

    def send_sq(dy, dv, slot):
        return pltpu.make_async_remote_copy(
            sq_mine,
            sq_all.at[slot],
            sq_s,
            sq_r,
            device_id={"occ": (y + dy) % ny, "vir": (v + dv) % (2 * nx)},
            device_id_type=MESH,
        )

    for slot, (dy, dv) in enumerate(others):
        send_sq(dy, dv, slot).start()
    for b in range(2):
        wide = amat[b, :, pl.ds(0, cols)].astype(jnp.float32)
        out[b] = (wide - gain[b] / (energy_gap(b) + LEVEL_SHIFT)).astype(jnp.bfloat16)
    pltpu.make_async_copy(sq_all, sq_all, sq_r).wait()
    total = jnp.sum(sq_all[...], axis=0) + sq_mine[...]
    total = jnp.broadcast_to(jnp.sum(total, axis=1, keepdims=True), (2, 128))
    counts = [(occ_pairs[z * 2 + b] * vir_pairs[z * 2 + b]).astype(jnp.float32) for b in range(2)]
    block = lax.broadcasted_iota(jnp.int32, (2, 128), 0)
    norm_out[...] = jnp.sqrt(total / jnp.where(block == 0, counts[0], counts[1]) + EPSILON)

    pltpu.make_async_copy(sq_all, sq_all, sq_s).wait()
    pltpu.make_async_copy(amp_peer, amp_peer, amp_s).wait()
    pltpu.make_async_copy(two_out, two_out, two_s).wait()
    for s in range(4):
        theirs = ladbuf.at[:, s, pl.ds(cols, cols), :]
        pltpu.make_async_copy(theirs, theirs, lad_s.at[s]).wait()
        pltpu.make_async_copy(msg_out.at[:, s], msg_out.at[:, s], one_s.at[s]).wait()


def body(amplitudes, ladder_ints, hole_ints, occ_energy, vir_energy, occ_pairs, vir_pairs):
    blocks, rows, cols = amplitudes.shape
    ny, nv = lax.axis_size("occ"), lax.axis_size("vir")
    nx = nv // 2
    tiles = (rows // 16) * (cols // 128) + 1
    vmem = pl.BlockSpec(memory_space=pltpu.VMEM)
    dma = pltpu.SemaphoreType.DMA
    updated, norm = pl.pallas_call(
        functools.partial(kernel, (nx, ny)),
        out_shape=(
            jax.ShapeDtypeStruct((blocks, rows, cols), jnp.bfloat16),
            jax.ShapeDtypeStruct((2, 128), jnp.float32),
        ),
        in_specs=[pl.BlockSpec(memory_space=pltpu.HBM)] * 7,
        out_specs=(vmem, vmem),
        scratch_shapes=[
            pltpu.SMEM(occ_pairs.shape, jnp.int32),
            pltpu.SMEM(vir_pairs.shape, jnp.int32),
            pltpu.VMEM(amplitudes.shape, amplitudes.dtype),
            pltpu.VMEM(hole_ints.shape, hole_ints.dtype),
            pltpu.VMEM(occ_energy.shape, jnp.float32),
            pltpu.VMEM(vir_energy.shape, jnp.float32),
            pltpu.VMEM((2, rows, cols), jnp.bfloat16),
            pltpu.VMEM((2, cols, cols), jnp.bfloat16),
            pltpu.VMEM((2, rows, 2 * cols), jnp.bfloat16),
            pltpu.VMEM((2, 4, 2 * cols, 4 * cols), jnp.bfloat16),
            pltpu.VMEM((2, 4, rows, 4 * cols), jnp.float32),
            pltpu.VMEM((2, rows, cols), jnp.float32),
            pltpu.VMEM((2, 4, 6, tiles, 8, 128), jnp.int16),
            pltpu.VMEM((2, 4, 6, tiles, 8, 128), jnp.int16),
            pltpu.VMEM((2, 6, tiles, 8, 128), jnp.int16),
            pltpu.VMEM((2, 6, tiles, 8, 128), jnp.int16),
            pltpu.VMEM((2, 128), jnp.float32),
            pltpu.VMEM((ny * nv - 1, 2, 128), jnp.float32),
            dma((6,)),
            dma((2,)),
            dma,
            dma((2,)),
            dma((4,)),
            dma((2, 4, 2)),
            dma((4,)),
            dma((2, 4, 3)),
            dma,
            dma((2, 3)),
            dma,
            dma,
        ],
        compiler_params=pltpu.CompilerParams(
            collective_id=0, has_side_effects=True, vmem_limit_bytes=55_500_000
        ),
    )(
        *(
            pltpu.with_memory_space_constraint(array, pltpu.HBM)
            for array in (occ_pairs, vir_pairs, amplitudes, hole_ints, occ_energy, vir_energy, ladder_ints)
        )
    )
    return updated, norm[:, 0]


def solution(mesh):
    in_specs = (
        P("irrep", None, ("occ", "vir")),
        P("irrep", ("occ", "vir"), None),
        P("irrep", None, None),
        P("irrep", None),
        P("irrep", ("occ", "vir")),
        P(),
        P(),
    )
    out_specs = (P("irrep", None, ("occ", "vir")), P("irrep"))
    return jax.shard_map(body, mesh=mesh, in_specs=in_specs, out_specs=out_specs, check_vma=False)
```

```python
import functools

import jax
import jax.numpy as jnp
from jax import lax
from jax.experimental import pallas as pl
from jax.experimental.pallas import tpu as pltpu
from jax.sharding import PartitionSpec as P

LEVEL_SHIFT = 0.5
EPSILON = 1e-06
MESH = pl.DeviceIdType.MESH
LEAD = 128
SPLIT = (slice(0, 1), slice(1, 4))
ORDER = ((0, 0), (1, 0), (2, 0), (0, 1), (3, 0), (1, 1), (2, 1), (3, 1))
REL = (2, 1, 3, 0)
STEPS_PER_OCTAVE = 128.0
CODE_RANGE = 32000.0
TINY = 1e-33


def kernel(
    dims,
    occ_pairs_hbm,
    vir_pairs_hbm,
    amp_hbm,
    hole_hbm,
    occ_e_hbm,
    vir_e_hbm,
    lad,
    out,
    norm_out,
    occ_pairs,
    vir_pairs,
    amp,
    hole,
    occ_e,
    vir_e,
    amp_peer,
    first,
    far_out,
    far_in,
    rear_out,
    rear_in,
    amat,
    ladbuf,
    part,
    gain,
    gap_of,
    msg_out,
    msg_in,
    two_out,
    two_in,
    sq_mine,
    sq_all,
    load_s,
    first_s,
    mine_s,
    late_r,
    far_s,
    far_r,
    amp_s,
    amp_r,
    lad_s,
    lad_r,
    one_s,
    one_r,
    two_s,
    last_r,
    two_r,
    sq_s,
    sq_r,
):
    nx, ny = dims
    rows, cols = amp.shape[1:]
    half = rows // 2
    lanes = cols // 128
    groups = half // 8
    whole = range(lanes)
    parts = (whole[: LEAD // 128], whole[LEAD // 128 :])
    z, y, v = lax.axis_index("irrep"), lax.axis_index("occ"), lax.axis_index("vir")
    x, c = v // 2, v % 2
    peer = {"vir": x * 2 + (1 - c)}
    size = {0: nx, 1: ny}

    def shifted(axis, by):
        if axis == 0:
            return {"vir": ((x + by) % nx) * 2 + c}
        return {"occ": (y + by) % ny}

    def columns(b, s, t, core):
        i, j = (x, y) if b == 0 else (y, x)
        to_i, to_j = (i + REL[t]) % 4, (j + REL[s]) % 4
        to_x, to_y = (to_i, to_j) if b == 0 else (to_j, to_i)
        return pl.ds(pl.multiple_of(((to_y * nx + to_x) * 2 + core) * cols, 128), cols)

    def load(n):
        src, dst = (
            (amp_hbm.at[0], amp.at[0]),
            (amp_hbm.at[1], amp.at[1]),
            (occ_pairs_hbm, occ_pairs),
            (vir_pairs_hbm, vir_pairs),
            (occ_e_hbm, occ_e),
            (vir_e_hbm, vir_e),
            (hole_hbm, hole),
        )[n]
        return pltpu.make_async_copy(src, dst, load_s.at[n])

    def load_first(b, n):
        width = LEAD if n == 0 else cols - LEAD
        at = pl.multiple_of(columns(b, 0, 0, 1 - c).start + n * LEAD, 128)
        return pltpu.make_async_copy(
            lad.at[b, :, pl.ds(at, width)], first.at[b, :, pl.ds(n * LEAD, width)], first_s.at[b, n]
        )

    def load_ladder(g):
        s, u = ORDER[g]
        for b in range(2):
            for t in range(4)[SPLIT[u]]:
                pltpu.make_async_copy(
                    lad.at[b, :, columns(b, s, t, c)],
                    ladbuf.at[b, s, pl.ds(0, cols), pl.ds(t * cols, cols)],
                    mine_s.at[b] if g == 0 else lad_r.at[b, 2 * s + u],
                ).start()

    def swap_first(b, part_no):
        where = pl.ds(LEAD * part_no, (cols - LEAD) * part_no + LEAD * (1 - part_no))
        return pltpu.make_async_remote_copy(
            first.at[b, :, where],
            ladbuf.at[b, 0, pl.ds(cols, cols), where],
            lad_s.at[0],
            lad_r.at[b, 0] if part_no == 0 else late_r.at[b],
            device_id=peer,
            device_id_type=MESH,
        )

    def swap_ladder(g):
        s, u = ORDER[g]
        for b in range(2):
            for t in range(4)[SPLIT[u]]:
                pltpu.make_async_remote_copy(
                    lad.at[b, :, columns(b, s, t, 1 - c)],
                    ladbuf.at[b, s, pl.ds(cols, cols), pl.ds(t * cols, cols)],
                    lad_s.at[s],
                    lad_r.at[b, 2 * s + u],
                    device_id=peer,
                    device_id_type=MESH,
                ).start()

    def swap_amp(b):
        return pltpu.make_async_remote_copy(
            amp.at[b], amp_peer.at[b], amp_s, amp_r.at[b], device_id=peer, device_id_type=MESH
        )

    for b in range(2):
        load(b).start()
    barrier = pltpu.get_barrier_semaphore()
    neighbours = [peer] + [shifted(axis, by) for axis in (0, 1) for by in (1, -1)]
    for device in neighbours:
        pl.semaphore_signal(barrier, inc=1, device_id=device, device_id_type=MESH)
    for n in range(2):
        for b in range(2):
            load_first(b, n).start()
    for n in (2, 3):
        load(n).start()
    load_ladder(0)
    pl.semaphore_wait(barrier, len(neighbours))
    for b in range(2):
        load(b).wait()
        swap_amp(b).start()
    for n in range(2):
        for b in range(2):
            load_first(b, n).wait()
            swap_first(b, n).start()
    load_ladder(1)
    swap_ladder(1)
    load_ladder(2)
    for n in (4, 5, 6):
        load(n).start()
    for n in (2, 3):
        load(n).wait()

    def keep(b, core, h=None):
        n_occ, n_vir = occ_pairs[z * 2 + b], vir_pairs[z * 2 + b]
        shape = (rows if h is None else half, cols)
        row = lax.broadcasted_iota(jnp.int32, shape, 0) + (0 if h is None else h * half)
        col = lax.broadcasted_iota(jnp.int32, shape, 1) + ((y * nx + x) * 2 + core) * cols
        return (row < n_occ) & (col < n_vir)

    def masked(values, b, core):
        return jnp.where(keep(b, core), values.astype(jnp.float32), 0.0)

    def local_terms(b):
        narrow = amat[b, :, pl.ds(0, cols)]
        occ_col = jnp.broadcast_to(occ_e[b : b + 1, :], (128, rows)).T
        gap = vir_e[b : b + 1, :] - jnp.concatenate([occ_col] * lanes, axis=1)
        gap_of[b] = gap
        hole_term = jnp.dot(hole[b], narrow, preferred_element_type=jnp.float32)
        gain[b] = hole_term + gap * narrow.astype(jnp.float32)

    def update(h):
        some = pl.ds(h * half, half)
        for b in range(2):
            wide = amat[b, some, pl.ds(0, cols)].astype(jnp.float32)
            out[b, some, :] = (wide - gain[b, some, :] / (gap_of[b, some, :] + LEVEL_SHIFT)).astype(jnp.bfloat16)

    def amplitudes(b):
        amat[b, :, pl.ds(0, cols)] = masked(amp[b], b, c).astype(jnp.bfloat16)
        swap_amp(b).wait_recv()
        amat[b, :, pl.ds(cols, cols)] = masked(amp_peer[b], b, 1 - c).astype(jnp.bfloat16)

    def encode(ref, message, blocks):
        biggest = None
        for k in blocks:
            here = jnp.max(jnp.abs(ref(k)[...]).reshape(groups, 8, 128), axis=0)
            biggest = here if biggest is None else jnp.maximum(biggest, here)
        code = jnp.ceil(jnp.log2(jnp.maximum(biggest, TINY)) * STEPS_PER_OCTAVE) + 1.0
        up = jnp.exp2(code * (-1.0 / STEPS_PER_OCTAVE)) * CODE_RANGE
        for n, k in enumerate(blocks):
            steps = jnp.round(ref(k)[...].reshape(groups, 8, 128) * up[None])
            message[pl.ds(n * groups, groups)] = steps.astype(jnp.int32).astype(jnp.int16)
        message[len(blocks) * groups] = code.astype(jnp.int32).astype(jnp.int16)

    def decoded(message, blocks):
        code = message[len(blocks) * groups].astype(jnp.int32).astype(jnp.float32)
        down = jnp.exp2(code * (1.0 / STEPS_PER_OCTAVE)) * (1.0 / CODE_RANGE)

        def read(k):
            at = pl.ds((k - blocks[0]) * groups, groups)
            steps = message[at].astype(jnp.int32).astype(jnp.float32)
            return (steps * down[None]).reshape(half, 128)

        return read

    def piece(b, s, t, h):
        def ref(k):
            return part.at[b, s, pl.ds(h * half, half), pl.ds(t * cols + k * 128, 128)]

        return ref

    def add_into(ref, messages, blocks):
        reads = [decoded(m, blocks) for m in messages]
        for k in blocks:
            total = ref(k)[...]
            for read in reads:
                total = total + read(k)
            ref(k)[...] = total

    def send_one(b, s, m):
        return pltpu.make_async_remote_copy(
            msg_out.at[b, s, m],
            msg_in.at[b, s, m],
            one_s.at[s],
            last_r.at[b, m - 2] if s == 3 and m > 1 else one_r.at[b, 2 * s - 2 + m if m < 2 else 6 + s],
            device_id=shifted(b, 1 - 2 * (m % 2)),
            device_id_type=MESH,
        )

    def send_two(b, m):
        return pltpu.make_async_remote_copy(
            two_out.at[b, m],
            two_in.at[b, m],
            two_s,
            two_r.at[b, m],
            device_id=shifted(1 - b, 1 - 2 * (m % 2)),
            device_id_type=MESH,
        )

    def send_far(b, d, n):
        return pltpu.make_async_remote_copy(
            (far_out, rear_out)[n].at[b, d],
            (far_in, rear_in)[n].at[b, d],
            far_s.at[n],
            far_r.at[b, d, n],
            device_id=shifted(b, 1 - 2 * d),
            device_id_type=MESH,
        )

    def stage_first():
        for b in range(2):
            amplitudes(b)
        for n in range(2):
            for b in range(2):
                own = ladbuf.at[b, 0, pl.ds(0, cols), pl.ds(0, cols)]
                if n == 0:
                    pltpu.make_async_copy(own, own, mine_s.at[b]).wait()
                swap_first(b, n).wait_recv()
                width = pl.ds(n * LEAD, len(parts[n]) * 128)
                part[b, 0, :, width] = jnp.dot(
                    amat[b], ladbuf[b, 0, :, width], preferred_element_type=jnp.float32
                )
                for d in range(2):
                    encode(piece(b, 0, 0, d), (far_out, rear_out)[n].at[b, d], parts[n])
                    send_far(b, d, n).start()

    def products(b, s, u):
        ts = range(4)[SPLIT[u]]
        width = pl.ds(ts[0] * cols, len(ts) * cols)
        both = ladbuf.at[b, s, :, width]
        pltpu.make_async_copy(both, both, lad_r.at[b, 2 * s + u]).wait()
        part[b, s, :, width] = jnp.dot(amat[b], ladbuf[b, s, :, width], preferred_element_type=jnp.float32)

    def emit(b, s, u):
        for d in range(2):
            t, h = (0, d) if u == 0 else (1 + d, 1 - d)
            encode(piece(b, s, t, h), msg_out.at[b, s, 2 * u + d], whole)
            send_one(b, s, 2 * u + d).start()

    def stage_a(s, u):
        for b in range(2):
            products(b, s, u)
            emit(b, s, u)

    def stage_b(s):
        for b in range(2):
            for d in range(2):
                if s == 0:
                    for n in range(2):
                        send_far(b, d, n).wait_recv()
                        add_into(piece(b, s, 1 + d, d), [(far_in, rear_in)[n].at[b, d]], parts[n])
                else:
                    send_one(b, s, d).wait_recv()
                    add_into(piece(b, s, 1 + d, d), [msg_in.at[b, s, d]], whole)
                encode(piece(b, s, 1 + d, d), msg_out.at[b, s, 4 + d], whole)
                send_one(b, s, 4 + d).start()

    def stage_c(s):
        for b in range(2):
            rest = msg_in.at[b, s, pl.ds(2, 4)]
            pltpu.make_async_copy(rest, rest, one_r.at[b, 6 + s]).wait()
            for d in range(2):
                add_into(piece(b, s, 3, d), [msg_in.at[b, s, m] for m in (4 + d, 3 - d)], whole)

    def two_first(m):
        at, h = ((0, 0), (0, 1), (1, 1), (2, 0))[m]
        for b in range(2):
            encode(piece(b, at, 3, h), two_out.at[b, m], whole)
            send_two(b, m).start()

    def two_second(m):
        for b in range(2):
            send_two(b, m).wait_recv()
            add_into(piece(b, 1 + m, 3, m), [two_in.at[b, m]], whole)
            encode(piece(b, 1 + m, 3, m), two_out.at[b, 4 + m], whole)
            send_two(b, 4 + m).start()

    stage_first()
    swap_ladder(2)
    load_ladder(3)
    stage_a(1, 0)
    swap_ladder(3)
    load_ladder(4)
    stage_a(2, 0)
    swap_ladder(4)
    load_ladder(5)
    stage_a(0, 1)
    stage_b(0)
    swap_ladder(5)
    load_ladder(6)
    stage_a(3, 0)
    stage_a(1, 1)
    swap_ladder(6)
    load_ladder(7)
    stage_b(1)
    stage_c(0)
    two_first(0)
    two_first(1)
    swap_ladder(7)
    stage_a(2, 1)
    stage_b(2)
    stage_c(1)
    two_first(2)
    for n in (4, 5, 6):
        load(n).wait()
    for b in range(2):
        products(b, 3, 1)
        local_terms(b)
    stage_b(3)
    two_second(0)
    for b in range(2):
        emit(b, 3, 1)
    stage_c(2)
    two_first(3)
    two_second(1)

    totals = [None, None]
    def add_one(b, h, m):
        send_one(b, 3, m).wait_recv()
        add_into(piece(b, 3, 3, h), [msg_in.at[b, 3, m]], whole)

    def add_two(b, h, m):
        send_two(b, m).wait_recv()
        add_into(piece(b, 3, 3, h), [two_in.at[b, m]], whole)

    def finish(b, h):
        some = pl.ds(h * half, half)
        ladder = part[b, 3, some, pl.ds(3 * cols, cols)]
        residual = jnp.where(keep(b, c, h), ladder + gain[b, some, :], 0.0)
        gain[b, some, :] = residual
        lane_sums = jnp.sum(residual * residual, axis=0, keepdims=True)
        for k in whole:
            here = lane_sums[:, k * 128 : (k + 1) * 128]
            totals[b] = here if totals[b] is None else totals[b] + here

    for b in range(2):
        add_one(b, 0, 4)
        add_two(b, 0, 4)
    for b in range(2):
        add_one(b, 1, 5)
        add_two(b, 1, 2)
    for b in range(2):
        add_one(b, 0, 3)
        add_two(b, 0, 3)
        finish(b, 0)
    update(0)
    for b in range(2):
        add_one(b, 1, 2)
        add_two(b, 1, 5)
        finish(b, 1)
    for b in range(2):
        sq_mine[pl.ds(b, 1), :] = totals[b]

    others = [(dy, dv) for dy in range(ny) for dv in range(2 * nx) if dy or dv]
    others.sort(key=lambda o: -(min(o[0], ny - o[0]) + min(o[1] // 2, nx - o[1] // 2)))

    def send_sq(dy, dv, slot):
        return pltpu.make_async_remote_copy(
            sq_mine,
            sq_all.at[slot],
            sq_s,
            sq_r,
            device_id={"occ": (y + dy) % ny, "vir": (v + dv) % (2 * nx)},
            device_id_type=MESH,
        )

    for slot, (dy, dv) in enumerate(others):
        send_sq(dy, dv, slot).start()
    update(1)
    pltpu.make_async_copy(amp_peer, amp_peer, amp_s).wait()
    pltpu.make_async_copy(two_out, two_out, two_s).wait()
    for n, lot in enumerate((far_out, rear_out)):
        pltpu.make_async_copy(lot, lot, far_s.at[n]).wait()
    for s in range(4):
        theirs = ladbuf.at[:, s, pl.ds(cols, cols), :]
        pltpu.make_async_copy(theirs, theirs, lad_s.at[s]).wait()
        sent = msg_out.at[:, s] if s else msg_out.at[:, s, pl.ds(2, 4)]
        pltpu.make_async_copy(sent, sent, one_s.at[s]).wait()
    pltpu.make_async_copy(sq_all, sq_all, sq_s).wait()
    pltpu.make_async_copy(sq_all, sq_all, sq_r).wait()
    total = jnp.sum(sq_all[...], axis=0) + sq_mine[...]
    total = jnp.broadcast_to(jnp.sum(total, axis=1, keepdims=True), (2, 128))
    counts = [(occ_pairs[z * 2 + b] * vir_pairs[z * 2 + b]).astype(jnp.float32) for b in range(2)]
    block = lax.broadcasted_iota(jnp.int32, (2, 128), 0)
    norm = jnp.sqrt(total / jnp.where(block == 0, counts[0], counts[1]) + EPSILON)
    lane = lax.broadcasted_iota(jnp.int32, (1, 128), 1)
    norm_out[...] = jnp.where(lane == 0, norm[:1, :], norm[1:, :]).reshape(128)


def body(amplitudes, ladder_ints, hole_ints, occ_energy, vir_energy, occ_pairs, vir_pairs):
    blocks, rows, cols = amplitudes.shape
    ny, nv = lax.axis_size("occ"), lax.axis_size("vir")
    nx = nv // 2
    tiles = (rows // 16) * (cols // 128) + 1
    lead = (rows // 16) * (LEAD // 128)
    vmem = pl.BlockSpec(memory_space=pltpu.VMEM)
    dma = pltpu.SemaphoreType.DMA
    updated, norm = pl.pallas_call(
        functools.partial(kernel, (nx, ny)),
        out_shape=(
            jax.ShapeDtypeStruct((blocks, rows, cols), jnp.bfloat16),
            jax.ShapeDtypeStruct((128,), jnp.float32),
        ),
        in_specs=[pl.BlockSpec(memory_space=pltpu.HBM)] * 7,
        out_specs=(vmem, vmem),
        scratch_shapes=[
            pltpu.SMEM(occ_pairs.shape, jnp.int32),
            pltpu.SMEM(vir_pairs.shape, jnp.int32),
            pltpu.VMEM(amplitudes.shape, amplitudes.dtype),
            pltpu.VMEM(hole_ints.shape, hole_ints.dtype),
            pltpu.VMEM(occ_energy.shape, jnp.float32),
            pltpu.VMEM(vir_energy.shape, jnp.float32),
            pltpu.VMEM((2, rows, cols), jnp.bfloat16),
            pltpu.VMEM((2, cols, cols), jnp.bfloat16),
            pltpu.VMEM((2, 2, lead + 1, 8, 128), jnp.int16),
            pltpu.VMEM((2, 2, lead + 1, 8, 128), jnp.int16),
            pltpu.VMEM((2, 2, tiles - lead, 8, 128), jnp.int16),
            pltpu.VMEM((2, 2, tiles - lead, 8, 128), jnp.int16),
            pltpu.VMEM((2, rows, 2 * cols), jnp.bfloat16),
            pltpu.VMEM((2, 4, 2 * cols, 4 * cols), jnp.bfloat16),
            pltpu.VMEM((2, 4, rows, 4 * cols), jnp.float32),
            pltpu.VMEM((2, rows, cols), jnp.float32),
            pltpu.VMEM((2, rows, cols), jnp.float32),
            pltpu.VMEM((2, 4, 6, tiles, 8, 128), jnp.int16),
            pltpu.VMEM((2, 4, 6, tiles, 8, 128), jnp.int16),
            pltpu.VMEM((2, 6, tiles, 8, 128), jnp.int16),
            pltpu.VMEM((2, 6, tiles, 8, 128), jnp.int16),
            pltpu.VMEM((2, 128), jnp.float32),
            pltpu.VMEM((ny * nv - 1, 2, 128), jnp.float32),
            dma((7,)),
            dma((2, 2)),
            dma((2,)),
            dma((2,)),
            dma((2,)),
            dma((2, 2, 2)),
            dma,
            dma((2,)),
            dma((4,)),
            dma((2, 8)),
            dma((4,)),
            dma((2, 9)),
            dma,
            dma((2, 4)),
            dma((2, 6)),
            dma,
            dma,
        ],
        compiler_params=pltpu.CompilerParams(
            collective_id=0, has_side_effects=True, vmem_limit_bytes=55_500_000
        ),
    )(
        *(
            pltpu.with_memory_space_constraint(array, pltpu.HBM)
            for array in (occ_pairs, vir_pairs, amplitudes, hole_ints, occ_energy, vir_energy, ladder_ints)
        )
    )
    return updated, norm[:2]


def solution(mesh):
    in_specs = (
        P("irrep", None, ("occ", "vir")),
        P("irrep", ("occ", "vir"), None),
        P("irrep", None, None),
        P("irrep", None),
        P("irrep", ("occ", "vir")),
        P(),
        P(),
    )
    out_specs = (P("irrep", None, ("occ", "vir")), P("irrep"))
    return jax.shard_map(body, mesh=mesh, in_specs=in_specs, out_specs=out_specs, check_vma=False)
```

```python
import functools

import jax
import jax.numpy as jnp
from jax import lax
from jax.experimental import pallas as pl
from jax.experimental.pallas import tpu as pltpu
from jax.sharding import PartitionSpec as P

LEVEL_SHIFT = 0.5
EPSILON = 1e-06
MESH = pl.DeviceIdType.MESH
LEAD = 128
SPLIT = (slice(0, 1), slice(1, 4))
ORDER = ((0, 0), (1, 0), (2, 0), (0, 1), (3, 0), (1, 1), (2, 1), (3, 1))
REL = (2, 1, 3, 0)
STEPS_PER_OCTAVE = 128.0
CODE_RANGE = 32000.0
TINY = 1e-33


def kernel(
    dims,
    occ_pairs_hbm,
    vir_pairs_hbm,
    amp_hbm,
    hole_hbm,
    occ_e_hbm,
    vir_e_hbm,
    lad,
    out,
    norm_out,
    occ_pairs,
    vir_pairs,
    amp,
    hole,
    occ_e,
    vir_e,
    amp_peer,
    first,
    far_out,
    far_in,
    rear_out,
    rear_in,
    amat,
    ladbuf,
    part,
    gain,
    gap_of,
    msg_out,
    msg_in,
    two_out,
    two_in,
    sq_mine,
    sq_all,
    load_s,
    first_s,
    mine_s,
    late_r,
    far_s,
    far_r,
    amp_s,
    amp_r,
    lad_s,
    lad_r,
    one_s,
    one_r,
    two_s,
    last_r,
    two_r,
    sq_s,
    sq_r,
):
    nx, ny = dims
    rows, cols = amp.shape[1:]
    half = rows // 2
    lanes = cols // 128
    groups = half // 8
    whole = range(lanes)
    parts = (whole[: LEAD // 128], whole[LEAD // 128 :])
    z, y, v = lax.axis_index("irrep"), lax.axis_index("occ"), lax.axis_index("vir")
    x, c = v // 2, v % 2
    peer = {"vir": x * 2 + (1 - c)}
    size = {0: nx, 1: ny}

    def shifted(axis, by):
        if axis == 0:
            return {"vir": ((x + by) % nx) * 2 + c}
        return {"occ": (y + by) % ny}

    def columns(b, s, t, core):
        i, j = (x, y) if b == 0 else (y, x)
        to_i, to_j = (i + REL[t]) % 4, (j + REL[s]) % 4
        to_x, to_y = (to_i, to_j) if b == 0 else (to_j, to_i)
        return pl.ds(pl.multiple_of(((to_y * nx + to_x) * 2 + core) * cols, 128), cols)

    def load(n):
        src, dst = (
            (amp_hbm.at[0], amp.at[0]),
            (amp_hbm.at[1], amp.at[1]),
            (occ_pairs_hbm, occ_pairs),
            (vir_pairs_hbm, vir_pairs),
            (occ_e_hbm, occ_e),
            (vir_e_hbm, vir_e),
            (hole_hbm, hole),
        )[n]
        return pltpu.make_async_copy(src, dst, load_s.at[n])

    def load_first(b, n):
        width = LEAD if n == 0 else cols - LEAD
        at = pl.multiple_of(columns(b, 0, 0, 1 - c).start + n * LEAD, 128)
        return pltpu.make_async_copy(
            lad.at[b, :, pl.ds(at, width)], first.at[b, :, pl.ds(n * LEAD, width)], first_s.at[b, n]
        )

    def load_ladder(g):
        s, u = ORDER[g]
        for b in range(2):
            for t in range(4)[SPLIT[u]]:
                pltpu.make_async_copy(
                    lad.at[b, :, columns(b, s, t, c)],
                    ladbuf.at[b, s, pl.ds(0, cols), pl.ds(t * cols, cols)],
                    mine_s.at[b] if g == 0 else lad_r.at[b, 2 * s + u],
                ).start()

    def swap_first(b, part_no):
        where = pl.ds(LEAD * part_no, (cols - LEAD) * part_no + LEAD * (1 - part_no))
        return pltpu.make_async_remote_copy(
            first.at[b, :, where],
            ladbuf.at[b, 0, pl.ds(cols, cols), where],
            lad_s.at[0],
            lad_r.at[b, 0] if part_no == 0 else late_r.at[b],
            device_id=peer,
            device_id_type=MESH,
        )

    def swap_ladder(g):
        s, u = ORDER[g]
        for b in range(2):
            for t in range(4)[SPLIT[u]]:
                pltpu.make_async_remote_copy(
                    lad.at[b, :, columns(b, s, t, 1 - c)],
                    ladbuf.at[b, s, pl.ds(cols, cols), pl.ds(t * cols, cols)],
                    lad_s.at[s],
                    lad_r.at[b, 2 * s + u],
                    device_id=peer,
                    device_id_type=MESH,
                ).start()

    def swap_amp(b):
        return pltpu.make_async_remote_copy(
            amp.at[b], amp_peer.at[b], amp_s, amp_r.at[b], device_id=peer, device_id_type=MESH
        )

    for b in range(2):
        load(b).start()
    barrier = pltpu.get_barrier_semaphore()
    neighbours = [peer] + [shifted(axis, by) for axis in (0, 1) for by in (1, -1)]
    for device in neighbours:
        pl.semaphore_signal(barrier, inc=1, device_id=device, device_id_type=MESH)
    for n in range(2):
        for b in range(2):
            load_first(b, n).start()
    for n in (2, 3):
        load(n).start()
    load_ladder(0)
    pl.semaphore_wait(barrier, len(neighbours))
    for n in range(2):
        for b in range(2):
            if n == 0:
                load(b).wait()
                swap_amp(b).start()
            load_first(b, n).wait()
            swap_first(b, n).start()
    load_ladder(1)
    swap_ladder(1)
    load_ladder(2)
    for n in (4, 5, 6):
        load(n).start()
    for n in (2, 3):
        load(n).wait()

    def keep(b, core, h=None):
        n_occ, n_vir = occ_pairs[z * 2 + b], vir_pairs[z * 2 + b]
        shape = (rows if h is None else half, cols)
        row = lax.broadcasted_iota(jnp.int32, shape, 0) + (0 if h is None else h * half)
        col = lax.broadcasted_iota(jnp.int32, shape, 1) + ((y * nx + x) * 2 + core) * cols
        return (row < n_occ) & (col < n_vir)

    def masked(values, b, core):
        return jnp.where(keep(b, core), values.astype(jnp.float32), 0.0)

    def local_terms(b):
        narrow = amat[b, :, pl.ds(0, cols)]
        occ_col = jnp.broadcast_to(occ_e[b : b + 1, :], (128, rows)).T
        gap = vir_e[b : b + 1, :] - jnp.concatenate([occ_col] * lanes, axis=1)
        gap_of[b] = gap
        hole_term = jnp.dot(hole[b], narrow, preferred_element_type=jnp.float32)
        gain[b] = hole_term + gap * narrow.astype(jnp.float32)

    def update(h):
        some = pl.ds(h * half, half)
        for b in range(2):
            wide = amat[b, some, pl.ds(0, cols)].astype(jnp.float32)
            out[b, some, :] = (wide - gain[b, some, :] / (gap_of[b, some, :] + LEVEL_SHIFT)).astype(jnp.bfloat16)

    def amplitudes(b):
        amat[b, :, pl.ds(0, cols)] = masked(amp[b], b, c).astype(jnp.bfloat16)
        swap_amp(b).wait_recv()
        amat[b, :, pl.ds(cols, cols)] = masked(amp_peer[b], b, 1 - c).astype(jnp.bfloat16)

    def encode(ref, message, blocks):
        biggest = None
        for k in blocks:
            here = jnp.max(jnp.abs(ref(k)[...]).reshape(groups, 8, 128), axis=0)
            biggest = here if biggest is None else jnp.maximum(biggest, here)
        code = jnp.ceil(jnp.log2(jnp.maximum(biggest, TINY)) * STEPS_PER_OCTAVE) + 1.0
        up = jnp.exp2(code * (-1.0 / STEPS_PER_OCTAVE)) * CODE_RANGE
        for n, k in enumerate(blocks):
            steps = jnp.round(ref(k)[...].reshape(groups, 8, 128) * up[None])
            message[pl.ds(n * groups, groups)] = steps.astype(jnp.int32).astype(jnp.int16)
        message[len(blocks) * groups] = code.astype(jnp.int32).astype(jnp.int16)

    def decoded(message, blocks):
        code = message[len(blocks) * groups].astype(jnp.int32).astype(jnp.float32)
        down = jnp.exp2(code * (1.0 / STEPS_PER_OCTAVE)) * (1.0 / CODE_RANGE)

        def read(k):
            at = pl.ds((k - blocks[0]) * groups, groups)
            steps = message[at].astype(jnp.int32).astype(jnp.float32)
            return (steps * down[None]).reshape(half, 128)

        return read

    def piece(b, s, t, h):
        def ref(k):
            return part.at[b, s, pl.ds(h * half, half), pl.ds(t * cols + k * 128, 128)]

        return ref

    def add_into(ref, messages, blocks):
        reads = [decoded(m, blocks) for m in messages]
        for k in blocks:
            total = ref(k)[...]
            for read in reads:
                total = total + read(k)
            ref(k)[...] = total

    def send_one(b, s, m):
        return pltpu.make_async_remote_copy(
            msg_out.at[b, s, m],
            msg_in.at[b, s, m],
            one_s.at[s],
            last_r.at[b, m - 2] if s == 3 and m > 1 else one_r.at[b, 2 * s - 2 + m if m < 2 else 6 + s],
            device_id=shifted(b, 1 - 2 * (m % 2)),
            device_id_type=MESH,
        )

    def send_two(b, m):
        return pltpu.make_async_remote_copy(
            two_out.at[b, m],
            two_in.at[b, m],
            two_s,
            two_r.at[b, m],
            device_id=shifted(1 - b, 1 - 2 * (m % 2)),
            device_id_type=MESH,
        )

    def send_far(b, d, n):
        return pltpu.make_async_remote_copy(
            (far_out, rear_out)[n].at[b, d],
            (far_in, rear_in)[n].at[b, d],
            far_s.at[n],
            far_r.at[b, d, n],
            device_id=shifted(b, 1 - 2 * d),
            device_id_type=MESH,
        )

    def stage_first():
        for n in range(2):
            for b in range(2):
                if n == 0:
                    amplitudes(b)
                own = ladbuf.at[b, 0, pl.ds(0, cols), pl.ds(0, cols)]
                if n == 0:
                    pltpu.make_async_copy(own, own, mine_s.at[b]).wait()
                swap_first(b, n).wait_recv()
                width = pl.ds(n * LEAD, len(parts[n]) * 128)
                part[b, 0, :, width] = jnp.dot(
                    amat[b], ladbuf[b, 0, :, width], preferred_element_type=jnp.float32
                )
                for d in range(2):
                    encode(piece(b, 0, 0, d), (far_out, rear_out)[n].at[b, d], parts[n])
                    send_far(b, d, n).start()

    def products(b, s, u):
        ts = range(4)[SPLIT[u]]
        width = pl.ds(ts[0] * cols, len(ts) * cols)
        both = ladbuf.at[b, s, :, width]
        pltpu.make_async_copy(both, both, lad_r.at[b, 2 * s + u]).wait()
        part[b, s, :, width] = jnp.dot(amat[b], ladbuf[b, s, :, width], preferred_element_type=jnp.float32)

    def emit(b, s, u):
        for d in range(2):
            t, h = (0, d) if u == 0 else (1 + d, 1 - d)
            encode(piece(b, s, t, h), msg_out.at[b, s, 2 * u + d], whole)
            send_one(b, s, 2 * u + d).start()

    def stage_a(s, u):
        for b in range(2):
            products(b, s, u)
            emit(b, s, u)

    def stage_b(s):
        for b in range(2):
            for d in range(2):
                if s == 0:
                    for n in range(2):
                        send_far(b, d, n).wait_recv()
                        add_into(piece(b, s, 1 + d, d), [(far_in, rear_in)[n].at[b, d]], parts[n])
                else:
                    send_one(b, s, d).wait_recv()
                    add_into(piece(b, s, 1 + d, d), [msg_in.at[b, s, d]], whole)
                encode(piece(b, s, 1 + d, d), msg_out.at[b, s, 4 + d], whole)
                send_one(b, s, 4 + d).start()

    def stage_c(s):
        for b in range(2):
            rest = msg_in.at[b, s, pl.ds(2, 4)]
            pltpu.make_async_copy(rest, rest, one_r.at[b, 6 + s]).wait()
            for d in range(2):
                add_into(piece(b, s, 3, d), [msg_in.at[b, s, m] for m in (4 + d, 3 - d)], whole)

    def two_first(m):
        at, h = ((0, 0), (0, 1), (1, 1), (2, 0))[m]
        for b in range(2):
            encode(piece(b, at, 3, h), two_out.at[b, m], whole)
            send_two(b, m).start()

    def two_second(m):
        for b in range(2):
            send_two(b, m).wait_recv()
            add_into(piece(b, 1 + m, 3, m), [two_in.at[b, m]], whole)
            encode(piece(b, 1 + m, 3, m), two_out.at[b, 4 + m], whole)
            send_two(b, 4 + m).start()

    stage_first()
    swap_ladder(2)
    load_ladder(3)
    stage_a(1, 0)
    swap_ladder(3)
    load_ladder(4)
    stage_a(2, 0)
    swap_ladder(4)
    load_ladder(5)
    stage_a(0, 1)
    stage_b(0)
    swap_ladder(5)
    load_ladder(6)
    stage_a(3, 0)
    stage_a(1, 1)
    swap_ladder(6)
    load_ladder(7)
    stage_b(1)
    stage_c(0)
    two_first(0)
    two_first(1)
    swap_ladder(7)
    stage_a(2, 1)
    stage_b(2)
    stage_c(1)
    two_first(2)
    for n in (4, 5, 6):
        load(n).wait()
    for b in range(2):
        products(b, 3, 1)
        local_terms(b)
    stage_b(3)
    two_second(0)
    for b in range(2):
        emit(b, 3, 1)
    stage_c(2)
    two_first(3)
    two_second(1)

    totals = [None, None]
    def add_one(b, h, m):
        send_one(b, 3, m).wait_recv()
        add_into(piece(b, 3, 3, h), [msg_in.at[b, 3, m]], whole)

    def add_two(b, h, m):
        send_two(b, m).wait_recv()
        add_into(piece(b, 3, 3, h), [two_in.at[b, m]], whole)

    def finish(b, h):
        some = pl.ds(h * half, half)
        ladder = part[b, 3, some, pl.ds(3 * cols, cols)]
        residual = jnp.where(keep(b, c, h), ladder + gain[b, some, :], 0.0)
        gain[b, some, :] = residual
        lane_sums = jnp.sum(residual * residual, axis=0, keepdims=True)
        for k in whole:
            here = lane_sums[:, k * 128 : (k + 1) * 128]
            totals[b] = here if totals[b] is None else totals[b] + here

    for b in range(2):
        add_one(b, 0, 4)
        add_two(b, 0, 4)
    for b in range(2):
        add_one(b, 1, 5)
        add_two(b, 1, 2)
    for b in range(2):
        add_one(b, 0, 3)
        add_two(b, 0, 3)
        finish(b, 0)
    update(0)
    for b in range(2):
        add_one(b, 1, 2)
        add_two(b, 1, 5)
        finish(b, 1)
    for b in range(2):
        sq_mine[pl.ds(b, 1), :] = totals[b]

    others = [(dy, dv) for dy in range(ny) for dv in range(2 * nx) if dy or dv]
    others.sort(key=lambda o: -(min(o[0], ny - o[0]) + min(o[1] // 2, nx - o[1] // 2)))

    def send_sq(dy, dv, slot):
        return pltpu.make_async_remote_copy(
            sq_mine,
            sq_all.at[slot],
            sq_s,
            sq_r,
            device_id={"occ": (y + dy) % ny, "vir": (v + dv) % (2 * nx)},
            device_id_type=MESH,
        )

    for slot, (dy, dv) in enumerate(others):
        send_sq(dy, dv, slot).start()
    update(1)
    pltpu.make_async_copy(amp_peer, amp_peer, amp_s).wait()
    pltpu.make_async_copy(two_out, two_out, two_s).wait()
    for n, lot in enumerate((far_out, rear_out)):
        pltpu.make_async_copy(lot, lot, far_s.at[n]).wait()
    for s in range(4):
        theirs = ladbuf.at[:, s, pl.ds(cols, cols), :]
        pltpu.make_async_copy(theirs, theirs, lad_s.at[s]).wait()
        sent = msg_out.at[:, s] if s else msg_out.at[:, s, pl.ds(2, 4)]
        pltpu.make_async_copy(sent, sent, one_s.at[s]).wait()
    pltpu.make_async_copy(sq_all, sq_all, sq_s).wait()
    pltpu.make_async_copy(sq_all, sq_all, sq_r).wait()
    total = jnp.sum(sq_all[...], axis=0) + sq_mine[...]
    total = jnp.broadcast_to(jnp.sum(total, axis=1, keepdims=True), (2, 128))
    counts = [(occ_pairs[z * 2 + b] * vir_pairs[z * 2 + b]).astype(jnp.float32) for b in range(2)]
    block = lax.broadcasted_iota(jnp.int32, (2, 128), 0)
    norm = jnp.sqrt(total / jnp.where(block == 0, counts[0], counts[1]) + EPSILON)
    lane = lax.broadcasted_iota(jnp.int32, (1, 128), 1)
    norm_out[...] = jnp.where(lane == 0, norm[:1, :], norm[1:, :]).reshape(128)


def body(amplitudes, ladder_ints, hole_ints, occ_energy, vir_energy, occ_pairs, vir_pairs):
    blocks, rows, cols = amplitudes.shape
    ny, nv = lax.axis_size("occ"), lax.axis_size("vir")
    nx = nv // 2
    tiles = (rows // 16) * (cols // 128) + 1
    lead = (rows // 16) * (LEAD // 128)
    vmem = pl.BlockSpec(memory_space=pltpu.VMEM)
    dma = pltpu.SemaphoreType.DMA
    updated, norm = pl.pallas_call(
        functools.partial(kernel, (nx, ny)),
        out_shape=(
            jax.ShapeDtypeStruct((blocks, rows, cols), jnp.bfloat16),
            jax.ShapeDtypeStruct((128,), jnp.float32),
        ),
        in_specs=[pl.BlockSpec(memory_space=pltpu.HBM)] * 7,
        out_specs=(vmem, vmem),
        scratch_shapes=[
            pltpu.SMEM(occ_pairs.shape, jnp.int32),
            pltpu.SMEM(vir_pairs.shape, jnp.int32),
            pltpu.VMEM(amplitudes.shape, amplitudes.dtype),
            pltpu.VMEM(hole_ints.shape, hole_ints.dtype),
            pltpu.VMEM(occ_energy.shape, jnp.float32),
            pltpu.VMEM(vir_energy.shape, jnp.float32),
            pltpu.VMEM((2, rows, cols), jnp.bfloat16),
            pltpu.VMEM((2, cols, cols), jnp.bfloat16),
            pltpu.VMEM((2, 2, lead + 1, 8, 128), jnp.int16),
            pltpu.VMEM((2, 2, lead + 1, 8, 128), jnp.int16),
            pltpu.VMEM((2, 2, tiles - lead, 8, 128), jnp.int16),
            pltpu.VMEM((2, 2, tiles - lead, 8, 128), jnp.int16),
            pltpu.VMEM((2, rows, 2 * cols), jnp.bfloat16),
            pltpu.VMEM((2, 4, 2 * cols, 4 * cols), jnp.bfloat16),
            pltpu.VMEM((2, 4, rows, 4 * cols), jnp.float32),
            pltpu.VMEM((2, rows, cols), jnp.float32),
            pltpu.VMEM((2, rows, cols), jnp.float32),
            pltpu.VMEM((2, 4, 6, tiles, 8, 128), jnp.int16),
            pltpu.VMEM((2, 4, 6, tiles, 8, 128), jnp.int16),
            pltpu.VMEM((2, 6, tiles, 8, 128), jnp.int16),
            pltpu.VMEM((2, 6, tiles, 8, 128), jnp.int16),
            pltpu.VMEM((2, 128), jnp.float32),
            pltpu.VMEM((ny * nv - 1, 2, 128), jnp.float32),
            dma((7,)),
            dma((2, 2)),
            dma((2,)),
            dma((2,)),
            dma((2,)),
            dma((2, 2, 2)),
            dma,
            dma((2,)),
            dma((4,)),
            dma((2, 8)),
            dma((4,)),
            dma((2, 9)),
            dma,
            dma((2, 4)),
            dma((2, 6)),
            dma,
            dma,
        ],
        compiler_params=pltpu.CompilerParams(
            collective_id=0, has_side_effects=True, vmem_limit_bytes=55_500_000
        ),
    )(
        *(
            pltpu.with_memory_space_constraint(array, pltpu.HBM)
            for array in (occ_pairs, vir_pairs, amplitudes, hole_ints, occ_energy, vir_energy, ladder_ints)
        )
    )
    return updated, norm[:2]


def solution(mesh):
    in_specs = (
        P("irrep", None, ("occ", "vir")),
        P("irrep", ("occ", "vir"), None),
        P("irrep", None, None),
        P("irrep", None),
        P("irrep", ("occ", "vir")),
        P(),
        P(),
    )
    out_specs = (P("irrep", None, ("occ", "vir")), P("irrep"))
    return jax.shard_map(body, mesh=mesh, in_specs=in_specs, out_specs=out_specs, check_vma=False)
```

```python
import functools

import jax
import jax.numpy as jnp
from jax import lax
from jax.experimental import pallas as pl
from jax.experimental.pallas import tpu as pltpu
from jax.sharding import PartitionSpec as P

LEVEL_SHIFT = 0.5
EPSILON = 1e-06
MESH = pl.DeviceIdType.MESH
LEAD = 128
SPLIT = (slice(0, 1), slice(1, 4))
ORDER = ((0, 0), (1, 0), (2, 0), (0, 1), (3, 0), (1, 1), (2, 1), (3, 1))
REL = (2, 1, 3, 0)
STEPS_PER_OCTAVE = 128.0
CODE_RANGE = 32000.0
TINY = 1e-33


def kernel(
    dims,
    occ_pairs_hbm,
    vir_pairs_hbm,
    amp_hbm,
    hole_hbm,
    occ_e_hbm,
    vir_e_hbm,
    lad,
    out,
    norm_out,
    occ_pairs,
    vir_pairs,
    amp,
    hole,
    occ_e,
    vir_e,
    amp_peer,
    first,
    far_out,
    far_in,
    rear_out,
    rear_in,
    amat,
    ladbuf,
    part,
    gain,
    gap_of,
    msg_out,
    msg_in,
    near_out,
    near_in,
    last_out,
    last_in,
    two_out,
    two_in,
    sq_mine,
    sq_all,
    load_s,
    first_s,
    mine_s,
    late_r,
    far_s,
    far_r,
    amp_s,
    amp_r,
    lad_s,
    lad_r,
    one_s,
    one_r,
    near_s,
    near_r,
    last_s,
    last_r,
    two_s,
    two_r,
    sq_s,
    sq_r,
):
    nx, ny = dims
    rows, cols = amp.shape[1:]
    half = rows // 2
    lanes = cols // 128
    groups = half // 8
    whole = range(lanes)
    parts = (whole[: LEAD // 128], whole[LEAD // 128 :])
    z, y, v = lax.axis_index("irrep"), lax.axis_index("occ"), lax.axis_index("vir")
    x, c = v // 2, v % 2
    peer = {"vir": x * 2 + (1 - c)}
    size = {0: nx, 1: ny}

    def shifted(axis, by):
        if axis == 0:
            return {"vir": ((x + by) % nx) * 2 + c}
        return {"occ": (y + by) % ny}

    def columns(b, s, t, core):
        i, j = (x, y) if b == 0 else (y, x)
        to_i, to_j = (i + REL[t]) % 4, (j + REL[s]) % 4
        to_x, to_y = (to_i, to_j) if b == 0 else (to_j, to_i)
        return pl.ds(pl.multiple_of(((to_y * nx + to_x) * 2 + core) * cols, 128), cols)

    def load(n):
        src, dst = (
            (amp_hbm.at[0], amp.at[0]),
            (amp_hbm.at[1], amp.at[1]),
            (occ_pairs_hbm, occ_pairs),
            (vir_pairs_hbm, vir_pairs),
            (occ_e_hbm, occ_e),
            (vir_e_hbm, vir_e),
            (hole_hbm, hole),
        )[n]
        return pltpu.make_async_copy(src, dst, load_s.at[n])

    def load_first(b, n):
        width = LEAD if n == 0 else cols - LEAD
        at = pl.multiple_of(columns(b, 0, 0, 1 - c).start + n * LEAD, 128)
        return pltpu.make_async_copy(
            lad.at[b, :, pl.ds(at, width)], first.at[b, :, pl.ds(n * LEAD, width)], first_s.at[b, n]
        )

    def load_ladder(g):
        s, u = ORDER[g]
        for b in range(2):
            for t in range(4)[SPLIT[u]]:
                pltpu.make_async_copy(
                    lad.at[b, :, columns(b, s, t, c)],
                    ladbuf.at[b, s, pl.ds(0, cols), pl.ds(t * cols, cols)],
                    mine_s.at[b] if g == 0 else lad_r.at[b, 2 * s + u],
                ).start()

    def swap_first(b, part_no):
        where = pl.ds(LEAD * part_no, (cols - LEAD) * part_no + LEAD * (1 - part_no))
        return pltpu.make_async_remote_copy(
            first.at[b, :, where],
            ladbuf.at[b, 0, pl.ds(cols, cols), where],
            lad_s,
            lad_r.at[b, 0] if part_no == 0 else late_r.at[b],
            device_id=peer,
            device_id_type=MESH,
        )

    def swap_ladder(g):
        s, u = ORDER[g]
        for b in range(2):
            for t in range(4)[SPLIT[u]]:
                pltpu.make_async_remote_copy(
                    lad.at[b, :, columns(b, s, t, 1 - c)],
                    ladbuf.at[b, s, pl.ds(cols, cols), pl.ds(t * cols, cols)],
                    lad_s,
                    lad_r.at[b, 2 * s + u],
                    device_id=peer,
                    device_id_type=MESH,
                ).start()

    def swap_amp(b):
        return pltpu.make_async_remote_copy(
            amp.at[b], amp_peer.at[b], amp_s, amp_r.at[b], device_id=peer, device_id_type=MESH
        )

    for b in range(2):
        load(b).start()
    barrier = pltpu.get_barrier_semaphore()
    neighbours = [peer] + [shifted(axis, by) for axis in (0, 1) for by in (1, -1)]
    for device in neighbours:
        pl.semaphore_signal(barrier, inc=1, device_id=device, device_id_type=MESH)
    for n in range(2):
        for b in range(2):
            load_first(b, n).start()
    for n in (2, 3):
        load(n).start()
    load_ladder(0)
    pl.semaphore_wait(barrier, len(neighbours))
    for n in range(2):
        for b in range(2):
            if n == 0:
                load(b).wait()
                swap_amp(b).start()
            load_first(b, n).wait()
            swap_first(b, n).start()
    load_ladder(1)
    swap_ladder(1)
    load_ladder(2)
    for n in (4, 5, 6):
        load(n).start()
    for n in (2, 3):
        load(n).wait()

    def keep(b, core, h=None):
        n_occ, n_vir = occ_pairs[z * 2 + b], vir_pairs[z * 2 + b]
        shape = (rows if h is None else half, cols)
        row = lax.broadcasted_iota(jnp.int32, shape, 0) + (0 if h is None else h * half)
        col = lax.broadcasted_iota(jnp.int32, shape, 1) + ((y * nx + x) * 2 + core) * cols
        return (row < n_occ) & (col < n_vir)

    def masked(values, b, core):
        return jnp.where(keep(b, core), values.astype(jnp.float32), 0.0)

    def local_terms(b):
        narrow = amat[b, :, pl.ds(0, cols)]
        occ_col = jnp.broadcast_to(occ_e[b : b + 1, :], (128, rows)).T
        gap = vir_e[b : b + 1, :] - jnp.concatenate([occ_col] * lanes, axis=1)
        gap_of[b] = gap
        hole_term = jnp.dot(hole[b], narrow, preferred_element_type=jnp.float32)
        gain[b] = hole_term + gap * narrow.astype(jnp.float32)

    def update(h):
        some = pl.ds(h * half, half)
        for b in range(2):
            wide = amat[b, some, pl.ds(0, cols)].astype(jnp.float32)
            out[b, some, :] = (wide - gain[b, some, :] / (gap_of[b, some, :] + LEVEL_SHIFT)).astype(jnp.bfloat16)

    def amplitudes(b):
        amat[b, :, pl.ds(0, cols)] = masked(amp[b], b, c).astype(jnp.bfloat16)
        swap_amp(b).wait_recv()
        amat[b, :, pl.ds(cols, cols)] = masked(amp_peer[b], b, 1 - c).astype(jnp.bfloat16)

    def encode(ref, message, blocks, second=None):
        tiles = [(ref, k) for k in blocks] + ([(second, k) for k in blocks] if second else [])
        biggest = None
        for source, k in tiles:
            here = jnp.max(jnp.abs(source(k)[...]).reshape(groups, 8, 128), axis=0)
            biggest = here if biggest is None else jnp.maximum(biggest, here)
        code = jnp.ceil(jnp.log2(jnp.maximum(biggest, TINY)) * STEPS_PER_OCTAVE) + 1.0
        up = jnp.exp2(code * (-1.0 / STEPS_PER_OCTAVE)) * CODE_RANGE
        for n, (source, k) in enumerate(tiles):
            steps = jnp.round(source(k)[...].reshape(groups, 8, 128) * up[None])
            message[pl.ds(n * groups, groups)] = steps.astype(jnp.int32).astype(jnp.int16)
        message[len(tiles) * groups] = code.astype(jnp.int32).astype(jnp.int16)

    def decoded(message, blocks, n=0, pieces=1):
        code = message[pieces * len(blocks) * groups].astype(jnp.int32).astype(jnp.float32)
        down = jnp.exp2(code * (1.0 / STEPS_PER_OCTAVE)) * (1.0 / CODE_RANGE)

        def read(k):
            at = pl.ds((n * len(blocks) + k - blocks[0]) * groups, groups)
            steps = message[at].astype(jnp.int32).astype(jnp.float32)
            return (steps * down[None]).reshape(half, 128)

        return read

    def piece(b, s, t, h):
        def ref(k):
            return part.at[b, s, pl.ds(h * half, half), pl.ds(t * cols + k * 128, 128)]

        return ref

    def add_into(ref, messages, blocks):
        reads = [decoded(m[0], blocks, *m[1:]) if isinstance(m, tuple) else decoded(m, blocks) for m in messages]
        for k in blocks:
            total = ref(k)[...]
            for read in reads:
                total = total + read(k)
            ref(k)[...] = total

    def send_one(b, s, m):
        at = (b, s - 1, m) if m < 2 else (b, m - 2)
        return pltpu.make_async_remote_copy(
            (msg_out if m < 2 else last_out).at[at],
            (msg_in if m < 2 else last_in).at[at],
            one_s if m < 2 else last_s,
            (one_r if m < 2 else last_r).at[at],
            device_id=shifted(b, 1 - 2 * (m % 2)),
            device_id_type=MESH,
        )

    def send_near(b, s, d):
        return pltpu.make_async_remote_copy(
            near_out.at[b, s, d],
            near_in.at[b, s, d],
            near_s,
            near_r.at[b, s],
            device_id=shifted(b, 1 - 2 * d),
            device_id_type=MESH,
        )

    def send_two(b, m):
        return pltpu.make_async_remote_copy(
            two_out.at[b, m],
            two_in.at[b, m],
            two_s,
            two_r.at[b, m],
            device_id=shifted(1 - b, 1 - 2 * (m % 2)),
            device_id_type=MESH,
        )

    def send_far(b, d, n):
        return pltpu.make_async_remote_copy(
            (far_out, rear_out)[n].at[b, d],
            (far_in, rear_in)[n].at[b, d],
            far_s.at[n],
            far_r.at[b, d, n],
            device_id=shifted(b, 1 - 2 * d),
            device_id_type=MESH,
        )

    def stage_first():
        for n in range(2):
            for b in range(2):
                if n == 0:
                    amplitudes(b)
                own = ladbuf.at[b, 0, pl.ds(0, cols), pl.ds(0, cols)]
                if n == 0:
                    pltpu.make_async_copy(own, own, mine_s.at[b]).wait()
                swap_first(b, n).wait_recv()
                width = pl.ds(n * LEAD, len(parts[n]) * 128)
                part[b, 0, :, width] = jnp.dot(
                    amat[b], ladbuf[b, 0, :, width], preferred_element_type=jnp.float32
                )
                for d in range(2):
                    encode(piece(b, 0, 0, d), (far_out, rear_out)[n].at[b, d], parts[n])
                    send_far(b, d, n).start()

    def products(b, s, u):
        ts = range(4)[SPLIT[u]]
        width = pl.ds(ts[0] * cols, len(ts) * cols)
        both = ladbuf.at[b, s, :, width]
        pltpu.make_async_copy(both, both, lad_r.at[b, 2 * s + u]).wait()
        part[b, s, :, width] = jnp.dot(amat[b], ladbuf[b, s, :, width], preferred_element_type=jnp.float32)

    def emit(b, s, u):
        for d in range(2):
            t, h = (0, d) if u == 0 else (1 + d, 1 - d)
            encode(piece(b, s, t, h), msg_out.at[b, s - 1, d] if u == 0 else last_out.at[b, d], whole)
            send_one(b, s, 2 * u + d).start()

    def stage_a(s, u):
        for b in range(2):
            products(b, s, u)
            if u == 0:
                emit(b, s, u)

    def stage_b(s):
        for b in range(2):
            for d in range(2):
                if s == 0:
                    for n in range(2):
                        send_far(b, d, n).wait_recv()
                        add_into(piece(b, s, 1 + d, d), [(far_in, rear_in)[n].at[b, d]], parts[n])
                else:
                    send_one(b, s, d).wait_recv()
                    add_into(piece(b, s, 1 + d, d), [msg_in.at[b, s - 1, d]], whole)
                if s == 3:
                    encode(piece(b, s, 1 + d, d), last_out.at[b, 2 + d], whole)
                    send_one(b, s, 4 + d).start()
                else:
                    encode(piece(b, s, 1 + d, 1 - d), near_out.at[b, s, d], whole, piece(b, s, 1 + d, d))
                    send_near(b, s, d).start()

    def stage_c(s):
        for b in range(2):
            pltpu.make_async_copy(near_in.at[b, s], near_in.at[b, s], near_r.at[b, s]).wait()
            for d in range(2):
                add_into(piece(b, s, 3, d), [(near_in.at[b, s, d], 1, 2), (near_in.at[b, s, 1 - d], 0, 2)], whole)

    def two_first(m):
        at, h = ((0, 0), (0, 1), (1, 1), (2, 0))[m]
        for b in range(2):
            encode(piece(b, at, 3, h), two_out.at[b, m], whole)
            send_two(b, m).start()

    def two_second(m):
        for b in range(2):
            send_two(b, m).wait_recv()
            add_into(piece(b, 1 + m, 3, m), [two_in.at[b, m]], whole)
            encode(piece(b, 1 + m, 3, m), two_out.at[b, 4 + m], whole)
            send_two(b, 4 + m).start()

    stage_first()
    swap_ladder(2)
    load_ladder(3)
    stage_a(1, 0)
    swap_ladder(3)
    load_ladder(4)
    stage_a(2, 0)
    swap_ladder(4)
    load_ladder(5)
    stage_a(0, 1)
    stage_b(0)
    swap_ladder(5)
    load_ladder(6)
    stage_a(3, 0)
    stage_a(1, 1)
    swap_ladder(6)
    load_ladder(7)
    stage_b(1)
    stage_c(0)
    two_first(0)
    two_first(1)
    swap_ladder(7)
    stage_a(2, 1)
    stage_b(2)
    stage_c(1)
    two_first(2)
    for n in (4, 5, 6):
        load(n).wait()
    for b in range(2):
        products(b, 3, 1)
        local_terms(b)
    stage_b(3)
    two_second(0)
    for b in range(2):
        emit(b, 3, 1)
    stage_c(2)
    two_first(3)
    two_second(1)

    totals = [None, None]
    def add_one(b, h, m):
        send_one(b, 3, m).wait_recv()
        add_into(piece(b, 3, 3, h), [last_in.at[b, m - 2]], whole)

    def add_two(b, h, m):
        send_two(b, m).wait_recv()
        add_into(piece(b, 3, 3, h), [two_in.at[b, m]], whole)

    def finish(b, h):
        some = pl.ds(h * half, half)
        ladder = part[b, 3, some, pl.ds(3 * cols, cols)]
        residual = jnp.where(keep(b, c, h), ladder + gain[b, some, :], 0.0)
        gain[b, some, :] = residual
        lane_sums = jnp.sum(residual * residual, axis=0, keepdims=True)
        for k in whole:
            here = lane_sums[:, k * 128 : (k + 1) * 128]
            totals[b] = here if totals[b] is None else totals[b] + here

    for b in range(2):
        add_one(b, 0, 4)
        add_two(b, 0, 4)
    for b in range(2):
        add_one(b, 1, 5)
        add_two(b, 1, 2)
    for b in range(2):
        add_one(b, 0, 3)
        add_two(b, 0, 3)
        finish(b, 0)
    update(0)
    for b in range(2):
        add_one(b, 1, 2)
        add_two(b, 1, 5)
        finish(b, 1)
    for b in range(2):
        sq_mine[pl.ds(b, 1), :] = totals[b]

    others = [(dy, dv) for dy in range(ny) for dv in range(2 * nx) if dy or dv]
    others.sort(key=lambda o: -(min(o[0], ny - o[0]) + min(o[1] // 2, nx - o[1] // 2)))

    def send_sq(dy, dv, slot):
        return pltpu.make_async_remote_copy(
            sq_mine,
            sq_all.at[slot],
            sq_s,
            sq_r,
            device_id={"occ": (y + dy) % ny, "vir": (v + dv) % (2 * nx)},
            device_id_type=MESH,
        )

    for slot, (dy, dv) in enumerate(others):
        send_sq(dy, dv, slot).start()
    update(1)
    pltpu.make_async_copy(amp_peer, amp_peer, amp_s).wait()
    pltpu.make_async_copy(two_out, two_out, two_s).wait()
    for n, lot in enumerate((far_out, rear_out)):
        pltpu.make_async_copy(lot, lot, far_s.at[n]).wait()
    theirs = ladbuf.at[:, :, pl.ds(cols, cols), :]
    pltpu.make_async_copy(theirs, theirs, lad_s).wait()
    for lot, sem in ((msg_out, one_s), (near_out, near_s), (last_out, last_s)):
        pltpu.make_async_copy(lot, lot, sem).wait()
    pltpu.make_async_copy(sq_all, sq_all, sq_s).wait()
    pltpu.make_async_copy(sq_all, sq_all, sq_r).wait()
    total = jnp.sum(sq_all[...], axis=0) + sq_mine[...]
    total = jnp.broadcast_to(jnp.sum(total, axis=1, keepdims=True), (2, 128))
    counts = [(occ_pairs[z * 2 + b] * vir_pairs[z * 2 + b]).astype(jnp.float32) for b in range(2)]
    block = lax.broadcasted_iota(jnp.int32, (2, 128), 0)
    norm = jnp.sqrt(total / jnp.where(block == 0, counts[0], counts[1]) + EPSILON)
    lane = lax.broadcasted_iota(jnp.int32, (1, 128), 1)
    norm_out[...] = jnp.where(lane == 0, norm[:1, :], norm[1:, :]).reshape(128)


def body(amplitudes, ladder_ints, hole_ints, occ_energy, vir_energy, occ_pairs, vir_pairs):
    blocks, rows, cols = amplitudes.shape
    ny, nv = lax.axis_size("occ"), lax.axis_size("vir")
    nx = nv // 2
    tiles = (rows // 16) * (cols // 128) + 1
    lead = (rows // 16) * (LEAD // 128)
    vmem = pl.BlockSpec(memory_space=pltpu.VMEM)
    dma = pltpu.SemaphoreType.DMA
    updated, norm = pl.pallas_call(
        functools.partial(kernel, (nx, ny)),
        out_shape=(
            jax.ShapeDtypeStruct((blocks, rows, cols), jnp.bfloat16),
            jax.ShapeDtypeStruct((128,), jnp.float32),
        ),
        in_specs=[pl.BlockSpec(memory_space=pltpu.HBM)] * 7,
        out_specs=(vmem, vmem),
        scratch_shapes=[
            pltpu.SMEM(occ_pairs.shape, jnp.int32),
            pltpu.SMEM(vir_pairs.shape, jnp.int32),
            pltpu.VMEM(amplitudes.shape, amplitudes.dtype),
            pltpu.VMEM(hole_ints.shape, hole_ints.dtype),
            pltpu.VMEM(occ_energy.shape, jnp.float32),
            pltpu.VMEM(vir_energy.shape, jnp.float32),
            pltpu.VMEM((2, rows, cols), jnp.bfloat16),
            pltpu.VMEM((2, cols, cols), jnp.bfloat16),
            pltpu.VMEM((2, 2, lead + 1, 8, 128), jnp.int16),
            pltpu.VMEM((2, 2, lead + 1, 8, 128), jnp.int16),
            pltpu.VMEM((2, 2, tiles - lead, 8, 128), jnp.int16),
            pltpu.VMEM((2, 2, tiles - lead, 8, 128), jnp.int16),
            pltpu.VMEM((2, rows, 2 * cols), jnp.bfloat16),
            pltpu.VMEM((2, 4, 2 * cols, 4 * cols), jnp.bfloat16),
            pltpu.VMEM((2, 4, rows, 4 * cols), jnp.float32),
            pltpu.VMEM((2, rows, cols), jnp.float32),
            pltpu.VMEM((2, rows, cols), jnp.float32),
            pltpu.VMEM((2, 3, 2, tiles, 8, 128), jnp.int16),
            pltpu.VMEM((2, 3, 2, tiles, 8, 128), jnp.int16),
            pltpu.VMEM((2, 3, 2, 2 * tiles - 1, 8, 128), jnp.int16),
            pltpu.VMEM((2, 3, 2, 2 * tiles - 1, 8, 128), jnp.int16),
            pltpu.VMEM((2, 4, tiles, 8, 128), jnp.int16),
            pltpu.VMEM((2, 4, tiles, 8, 128), jnp.int16),
            pltpu.VMEM((2, 6, tiles, 8, 128), jnp.int16),
            pltpu.VMEM((2, 6, tiles, 8, 128), jnp.int16),
            pltpu.VMEM((2, 128), jnp.float32),
            pltpu.VMEM((ny * nv - 1, 2, 128), jnp.float32),
            dma((7,)),
            dma((2, 2)),
            dma((2,)),
            dma((2,)),
            dma((2,)),
            dma((2, 2, 2)),
            dma,
            dma((2,)),
            dma,
            dma((2, 8)),
            dma,
            dma((2, 3, 2)),
            dma,
            dma((2, 3)),
            dma,
            dma((2, 4)),
            dma,
            dma((2, 6)),
            dma,
            dma,
        ],
        compiler_params=pltpu.CompilerParams(
            collective_id=0, has_side_effects=True, vmem_limit_bytes=55_500_000
        ),
    )(
        *(
            pltpu.with_memory_space_constraint(array, pltpu.HBM)
            for array in (occ_pairs, vir_pairs, amplitudes, hole_ints, occ_energy, vir_energy, ladder_ints)
        )
    )
    return updated, norm[:2]


def solution(mesh):
    in_specs = (
        P("irrep", None, ("occ", "vir")),
        P("irrep", ("occ", "vir"), None),
        P("irrep", None, None),
        P("irrep", None),
        P("irrep", ("occ", "vir")),
        P(),
        P(),
    )
    out_specs = (P("irrep", None, ("occ", "vir")), P("irrep"))
    return jax.shard_map(body, mesh=mesh, in_specs=in_specs, out_specs=out_specs, check_vma=False)
```

```python
import functools

import jax
import jax.numpy as jnp
from jax import lax
from jax.experimental import pallas as pl
from jax.experimental.pallas import tpu as pltpu
from jax.sharding import PartitionSpec as P

LEVEL_SHIFT = 0.5
EPSILON = 1e-06
MESH = pl.DeviceIdType.MESH
LEAD = 128
SPLIT = (slice(0, 1), slice(1, 4))
ORDER = ((0, 0), (1, 0), (2, 0), (0, 1), (3, 0), (1, 1), (2, 1), (3, 1))
REL = (2, 1, 3, 0)
STEPS_PER_OCTAVE = 128.0
CODE_RANGE = 32000.0
TINY = 1e-33


def kernel(
    dims,
    occ_pairs_hbm,
    vir_pairs_hbm,
    amp_hbm,
    hole_hbm,
    occ_e_hbm,
    vir_e_hbm,
    lad,
    out,
    norm_out,
    occ_pairs,
    vir_pairs,
    amp,
    hole,
    occ_e,
    vir_e,
    amp_peer,
    first,
    far_out,
    far_in,
    rear_out,
    rear_in,
    amat,
    ladbuf,
    part,
    gain,
    gap_of,
    msg_out,
    msg_in,
    near_out,
    near_in,
    last_out,
    last_in,
    two_out,
    two_in,
    sq_mine,
    sq_all,
    load_s,
    first_s,
    mine_s,
    late_r,
    far_s,
    far_r,
    amp_s,
    amp_r,
    lad_s,
    lad_r,
    one_s,
    one_r,
    near_s,
    near_r,
    last_s,
    last_r,
    two_s,
    two_r,
    sq_s,
    sq_r,
):
    nx, ny = dims
    rows, cols = amp.shape[1:]
    half = rows // 2
    lanes = cols // 128
    groups = half // 8
    whole = range(lanes)
    parts = (whole[: LEAD // 128], whole[LEAD // 128 :])
    z, y, v = lax.axis_index("irrep"), lax.axis_index("occ"), lax.axis_index("vir")
    x, c = v // 2, v % 2
    peer = {"vir": x * 2 + (1 - c)}
    size = {0: nx, 1: ny}

    def shifted(axis, by):
        if axis == 0:
            return {"vir": ((x + by) % nx) * 2 + c}
        return {"occ": (y + by) % ny}

    def columns(b, s, t, core):
        i, j = (x, y) if b == 0 else (y, x)
        to_i, to_j = (i + REL[t]) % 4, (j + REL[s]) % 4
        to_x, to_y = (to_i, to_j) if b == 0 else (to_j, to_i)
        return pl.ds(pl.multiple_of(((to_y * nx + to_x) * 2 + core) * cols, 128), cols)

    def load(n):
        src, dst = (
            (amp_hbm.at[0], amp.at[0]),
            (amp_hbm.at[1], amp.at[1]),
            (occ_pairs_hbm, occ_pairs),
            (vir_pairs_hbm, vir_pairs),
            (occ_e_hbm, occ_e),
            (vir_e_hbm, vir_e),
            (hole_hbm, hole),
        )[n]
        return pltpu.make_async_copy(src, dst, load_s.at[n])

    def load_first(b, n):
        width = LEAD if n == 0 else cols - LEAD
        at = pl.multiple_of(columns(b, 0, 0, 1 - c).start + n * LEAD, 128)
        return pltpu.make_async_copy(
            lad.at[b, :, pl.ds(at, width)], first.at[b, :, pl.ds(n * LEAD, width)], first_s.at[b, n]
        )

    def load_ladder(g):
        s, u = ORDER[g]
        for b in range(2):
            for t in range(4)[SPLIT[u]]:
                pltpu.make_async_copy(
                    lad.at[b, :, columns(b, s, t, c)],
                    ladbuf.at[b, s, pl.ds(0, cols), pl.ds(t * cols, cols)],
                    mine_s.at[b] if g == 0 else lad_r.at[b, 2 * s + u],
                ).start()

    def swap_first(b, part_no):
        where = pl.ds(LEAD * part_no, (cols - LEAD) * part_no + LEAD * (1 - part_no))
        return pltpu.make_async_remote_copy(
            first.at[b, :, where],
            ladbuf.at[b, 0, pl.ds(cols, cols), where],
            lad_s,
            lad_r.at[b, 0] if part_no == 0 else late_r.at[b],
            device_id=peer,
            device_id_type=MESH,
        )

    def swap_ladder(g):
        s, u = ORDER[g]
        for b in range(2):
            for t in range(4)[SPLIT[u]]:
                pltpu.make_async_remote_copy(
                    lad.at[b, :, columns(b, s, t, 1 - c)],
                    ladbuf.at[b, s, pl.ds(cols, cols), pl.ds(t * cols, cols)],
                    lad_s,
                    lad_r.at[b, 2 * s + u],
                    device_id=peer,
                    device_id_type=MESH,
                ).start()

    def swap_amp(b):
        return pltpu.make_async_remote_copy(
            amp.at[b], amp_peer.at[b], amp_s, amp_r.at[b], device_id=peer, device_id_type=MESH
        )

    for b in range(2):
        load(b).start()
    barrier = pltpu.get_barrier_semaphore()
    neighbours = [peer] + [shifted(axis, by) for axis in (0, 1) for by in (1, -1)]
    for device in neighbours:
        pl.semaphore_signal(barrier, inc=1, device_id=device, device_id_type=MESH)
    for n in range(2):
        for b in range(2):
            load_first(b, n).start()
    for n in (2, 3):
        load(n).start()
    load_ladder(0)
    pl.semaphore_wait(barrier, len(neighbours))
    for n in range(2):
        for b in range(2):
            if n == 0:
                load(b).wait()
                swap_amp(b).start()
            load_first(b, n).wait()
            swap_first(b, n).start()
    load_ladder(1)
    swap_ladder(1)
    load_ladder(2)
    for n in (4, 5, 6):
        load(n).start()
    for n in (2, 3):
        load(n).wait()

    def keep(b, core, h=None):
        n_occ, n_vir = occ_pairs[z * 2 + b], vir_pairs[z * 2 + b]
        shape = (rows if h is None else half, cols)
        row = lax.broadcasted_iota(jnp.int32, shape, 0) + (0 if h is None else h * half)
        col = lax.broadcasted_iota(jnp.int32, shape, 1) + ((y * nx + x) * 2 + core) * cols
        return (row < n_occ) & (col < n_vir)

    def masked(values, b, core):
        return jnp.where(keep(b, core), values.astype(jnp.float32), 0.0)

    def local_terms(b):
        narrow = amat[b, :, pl.ds(0, cols)]
        occ_col = jnp.broadcast_to(occ_e[b : b + 1, :], (128, rows)).T
        gap = vir_e[b : b + 1, :] - jnp.concatenate([occ_col] * lanes, axis=1)
        gap_of[b] = gap
        hole_term = jnp.dot(hole[b], narrow, preferred_element_type=jnp.float32)
        gain[b] = hole_term + gap * narrow.astype(jnp.float32)

    def update(h):
        some = pl.ds(h * half, half)
        for b in range(2):
            wide = amat[b, some, pl.ds(0, cols)].astype(jnp.float32)
            out[b, some, :] = (wide - gain[b, some, :] / (gap_of[b, some, :] + LEVEL_SHIFT)).astype(jnp.bfloat16)

    def amplitudes(b):
        amat[b, :, pl.ds(0, cols)] = masked(amp[b], b, c).astype(jnp.bfloat16)
        swap_amp(b).wait_recv()
        amat[b, :, pl.ds(cols, cols)] = masked(amp_peer[b], b, 1 - c).astype(jnp.bfloat16)

    def encode(ref, message, blocks, second=None):
        tiles = [(ref, k) for k in blocks] + ([(second, k) for k in blocks] if second else [])
        biggest = None
        for source, k in tiles:
            here = jnp.max(jnp.abs(source(k)[...]).reshape(groups, 8, 128), axis=0)
            biggest = here if biggest is None else jnp.maximum(biggest, here)
        code = jnp.ceil(jnp.log2(jnp.maximum(biggest, TINY)) * STEPS_PER_OCTAVE) + 1.0
        up = jnp.exp2(code * (-1.0 / STEPS_PER_OCTAVE)) * CODE_RANGE
        for n, (source, k) in enumerate(tiles):
            steps = jnp.round(source(k)[...].reshape(groups, 8, 128) * up[None])
            message[pl.ds(n * groups, groups)] = steps.astype(jnp.int32).astype(jnp.int16)
        message[len(tiles) * groups] = code.astype(jnp.int32).astype(jnp.int16)

    def decoded(message, blocks, n=0, pieces=1):
        code = message[pieces * len(blocks) * groups].astype(jnp.int32).astype(jnp.float32)
        down = jnp.exp2(code * (1.0 / STEPS_PER_OCTAVE)) * (1.0 / CODE_RANGE)

        def read(k):
            at = pl.ds((n * len(blocks) + k - blocks[0]) * groups, groups)
            steps = message[at].astype(jnp.int32).astype(jnp.float32)
            return (steps * down[None]).reshape(half, 128)

        return read

    def piece(b, s, t, h):
        def ref(k):
            return part.at[b, s, pl.ds(h * half, half), pl.ds(t * cols + k * 128, 128)]

        return ref

    def add_into(ref, messages, blocks):
        reads = [decoded(m[0], blocks, *m[1:]) if isinstance(m, tuple) else decoded(m, blocks) for m in messages]
        for k in blocks:
            total = ref(k)[...]
            for read in reads:
                total = total + read(k)
            ref(k)[...] = total

    def send_one(b, s, m):
        at = (b, s - 1, m) if m < 2 else (b, m - 2)
        return pltpu.make_async_remote_copy(
            (msg_out if m < 2 else last_out).at[at],
            (msg_in if m < 2 else last_in).at[at],
            one_s if m < 2 else last_s,
            (one_r if m < 2 else last_r).at[at],
            device_id=shifted(b, 1 - 2 * (m % 2)),
            device_id_type=MESH,
        )

    def send_near(b, s, d):
        return pltpu.make_async_remote_copy(
            near_out.at[b, s, d],
            near_in.at[b, s, d],
            near_s,
            near_r.at[b, s],
            device_id=shifted(b, 1 - 2 * d),
            device_id_type=MESH,
        )

    def send_two(b, m):
        return pltpu.make_async_remote_copy(
            two_out.at[b, m],
            two_in.at[b, m],
            two_s,
            two_r.at[b, m],
            device_id=shifted(1 - b, 1 - 2 * (m % 2)),
            device_id_type=MESH,
        )

    def send_far(b, d, n):
        return pltpu.make_async_remote_copy(
            (far_out, rear_out)[n].at[b, d],
            (far_in, rear_in)[n].at[b, d],
            far_s.at[n],
            far_r.at[b, d, n],
            device_id=shifted(b, 1 - 2 * d),
            device_id_type=MESH,
        )

    def stage_first():
        for n in range(2):
            for b in range(2):
                if n == 0:
                    amplitudes(b)
                own = ladbuf.at[b, 0, pl.ds(0, cols), pl.ds(0, cols)]
                if n == 0:
                    pltpu.make_async_copy(own, own, mine_s.at[b]).wait()
                swap_first(b, n).wait_recv()
                width = pl.ds(n * LEAD, len(parts[n]) * 128)
                part[b, 0, :, width] = jnp.dot(
                    amat[b], ladbuf[b, 0, :, width], preferred_element_type=jnp.float32
                )
                for d in range(2):
                    encode(piece(b, 0, 0, d), (far_out, rear_out)[n].at[b, d], parts[n])
                    send_far(b, d, n).start()

    def products(b, s, u):
        ts = range(4)[SPLIT[u]]
        width = pl.ds(ts[0] * cols, len(ts) * cols)
        both = ladbuf.at[b, s, :, width]
        pltpu.make_async_copy(both, both, lad_r.at[b, 2 * s + u]).wait()
        part[b, s, :, width] = jnp.dot(amat[b], ladbuf[b, s, :, width], preferred_element_type=jnp.float32)

    def emit(b, s, u):
        for d in range(2):
            t, h = (0, d) if u == 0 else (1 + d, 1 - d)
            encode(piece(b, s, t, h), msg_out.at[b, s - 1, d] if u == 0 else last_out.at[b, d], whole)
            send_one(b, s, 2 * u + d).start()

    def stage_a(s, u):
        for b in range(2):
            products(b, s, u)
            if u == 0:
                emit(b, s, u)

    def stage_b(s):
        for b in range(2):
            for d in range(2):
                if s == 0:
                    for n in range(2):
                        send_far(b, d, n).wait_recv()
                        add_into(piece(b, s, 1 + d, d), [(far_in, rear_in)[n].at[b, d]], parts[n])
                else:
                    send_one(b, s, d).wait_recv()
                    add_into(piece(b, s, 1 + d, d), [msg_in.at[b, s - 1, d]], whole)
                if s == 3:
                    encode(piece(b, s, 1 + d, d), last_out.at[b, 2 + d], whole)
                    send_one(b, s, 4 + d).start()
                else:
                    encode(piece(b, s, 1 + d, 1 - d), near_out.at[b, s, d], whole, piece(b, s, 1 + d, d))
                    send_near(b, s, d).start()

    def stage_c(s):
        for b in range(2):
            pltpu.make_async_copy(near_in.at[b, s], near_in.at[b, s], near_r.at[b, s]).wait()
            for d in range(2):
                add_into(piece(b, s, 3, d), [(near_in.at[b, s, d], 1, 2), (near_in.at[b, s, 1 - d], 0, 2)], whole)

    def two_first(m):
        at, h = ((0, 0), (0, 1), (1, 1), (2, 0))[m]
        for b in range(2):
            encode(piece(b, at, 3, h), two_out.at[b, m], whole)
            send_two(b, m).start()

    def two_second(m):
        for b in range(2):
            send_two(b, m).wait_recv()
            add_into(piece(b, 1 + m, 3, m), [two_in.at[b, m]], whole)
            encode(piece(b, 1 + m, 3, m), two_out.at[b, 4 + m], whole)
            send_two(b, 4 + m).start()

    stage_first()
    swap_ladder(2)
    load_ladder(3)
    stage_a(1, 0)
    swap_ladder(3)
    load_ladder(4)
    stage_a(2, 0)
    swap_ladder(4)
    load_ladder(5)
    stage_a(0, 1)
    stage_b(0)
    swap_ladder(5)
    load_ladder(6)
    stage_a(3, 0)
    stage_a(1, 1)
    swap_ladder(6)
    load_ladder(7)
    stage_b(1)
    stage_c(0)
    two_first(0)
    two_first(1)
    swap_ladder(7)
    stage_a(2, 1)
    stage_b(2)
    stage_c(1)
    two_first(2)
    for n in (4, 5, 6):
        load(n).wait()
    for b in range(2):
        products(b, 3, 1)
        local_terms(b)
    stage_b(3)
    two_second(0)
    for b in range(2):
        emit(b, 3, 1)
    stage_c(2)
    two_first(3)
    two_second(1)

    totals = [None, None]
    def add_one(b, h, m):
        send_one(b, 3, m).wait_recv()
        add_into(piece(b, 3, 3, h), [last_in.at[b, m - 2]], whole)

    def add_two(b, h, m):
        send_two(b, m).wait_recv()
        add_into(piece(b, 3, 3, h), [two_in.at[b, m]], whole)

    def finish(b, h):
        some = pl.ds(h * half, half)
        ladder = part[b, 3, some, pl.ds(3 * cols, cols)]
        residual = jnp.where(keep(b, c, h), ladder + gain[b, some, :], 0.0)
        gain[b, some, :] = residual
        lane_sums = jnp.sum(residual * residual, axis=0, keepdims=True)
        for k in whole:
            here = lane_sums[:, k * 128 : (k + 1) * 128]
            totals[b] = here if totals[b] is None else totals[b] + here

    for b in range(2):
        add_one(b, 0, 4)
        add_two(b, 0, 4)
    for b in range(2):
        add_one(b, 1, 5)
        add_two(b, 1, 2)
    for b in range(2):
        add_one(b, 0, 3)
        add_two(b, 0, 3)
        finish(b, 0)
    update(0)
    for b in range(2):
        add_one(b, 1, 2)
        add_two(b, 1, 5)
        finish(b, 1)
    for b in range(2):
        sq_mine[pl.ds(b, 1), :] = totals[b]

    others = [(dy, dv) for dy in range(ny) for dv in range(2 * nx) if dy or dv]
    others.sort(key=lambda o: -(min(o[0], ny - o[0]) + min(o[1] // 2, nx - o[1] // 2)))

    def send_sq(dy, dv, slot):
        return pltpu.make_async_remote_copy(
            sq_mine,
            sq_all.at[slot],
            sq_s,
            sq_r,
            device_id={"occ": (y + dy) % ny, "vir": (v + dv) % (2 * nx)},
            device_id_type=MESH,
        )

    for slot, (dy, dv) in enumerate(others):
        send_sq(dy, dv, slot).start()
    update(1)
    pltpu.make_async_copy(amp_peer, amp_peer, amp_s).wait()
    pltpu.make_async_copy(two_out, two_out, two_s).wait()
    for n, lot in enumerate((far_out, rear_out)):
        pltpu.make_async_copy(lot, lot, far_s.at[n]).wait()
    theirs = ladbuf.at[:, :, pl.ds(cols, cols), :]
    pltpu.make_async_copy(theirs, theirs, lad_s).wait()
    for lot, sem in ((msg_out, one_s), (near_out, near_s), (last_out, last_s)):
        pltpu.make_async_copy(lot, lot, sem).wait()
    pltpu.make_async_copy(sq_all, sq_all, sq_s).wait()
    pltpu.make_async_copy(sq_all, sq_all, sq_r).wait()
    total = jnp.sum(sq_all[...], axis=0) + sq_mine[...]
    total = jnp.broadcast_to(jnp.sum(total, axis=1, keepdims=True), (2, 128))
    counts = [(occ_pairs[z * 2 + b] * vir_pairs[z * 2 + b]).astype(jnp.float32) for b in range(2)]
    block = lax.broadcasted_iota(jnp.int32, (2, 128), 0)
    norm = jnp.sqrt(total / jnp.where(block == 0, counts[0], counts[1]) + EPSILON)
    for b in range(2):
        norm_out[b] = norm[b, 0]


def body(amplitudes, ladder_ints, hole_ints, occ_energy, vir_energy, occ_pairs, vir_pairs):
    blocks, rows, cols = amplitudes.shape
    ny, nv = lax.axis_size("occ"), lax.axis_size("vir")
    nx = nv // 2
    tiles = (rows // 16) * (cols // 128) + 1
    lead = (rows // 16) * (LEAD // 128)
    vmem = pl.BlockSpec(memory_space=pltpu.VMEM)
    dma = pltpu.SemaphoreType.DMA
    updated, norm = pl.pallas_call(
        functools.partial(kernel, (nx, ny)),
        out_shape=(
            jax.ShapeDtypeStruct((blocks, rows, cols), jnp.bfloat16),
            jax.ShapeDtypeStruct((2,), jnp.float32),
        ),
        in_specs=[pl.BlockSpec(memory_space=pltpu.HBM)] * 7,
        out_specs=(vmem, pl.BlockSpec(memory_space=pltpu.SMEM)),
        scratch_shapes=[
            pltpu.SMEM(occ_pairs.shape, jnp.int32),
            pltpu.SMEM(vir_pairs.shape, jnp.int32),
            pltpu.VMEM(amplitudes.shape, amplitudes.dtype),
            pltpu.VMEM(hole_ints.shape, hole_ints.dtype),
            pltpu.VMEM(occ_energy.shape, jnp.float32),
            pltpu.VMEM(vir_energy.shape, jnp.float32),
            pltpu.VMEM((2, rows, cols), jnp.bfloat16),
            pltpu.VMEM((2, cols, cols), jnp.bfloat16),
            pltpu.VMEM((2, 2, lead + 1, 8, 128), jnp.int16),
            pltpu.VMEM((2, 2, lead + 1, 8, 128), jnp.int16),
            pltpu.VMEM((2, 2, tiles - lead, 8, 128), jnp.int16),
            pltpu.VMEM((2, 2, tiles - lead, 8, 128), jnp.int16),
            pltpu.VMEM((2, rows, 2 * cols), jnp.bfloat16),
            pltpu.VMEM((2, 4, 2 * cols, 4 * cols), jnp.bfloat16),
            pltpu.VMEM((2, 4, rows, 4 * cols), jnp.float32),
            pltpu.VMEM((2, rows, cols), jnp.float32),
            pltpu.VMEM((2, rows, cols), jnp.float32),
            pltpu.VMEM((2, 3, 2, tiles, 8, 128), jnp.int16),
            pltpu.VMEM((2, 3, 2, tiles, 8, 128), jnp.int16),
            pltpu.VMEM((2, 3, 2, 2 * tiles - 1, 8, 128), jnp.int16),
            pltpu.VMEM((2, 3, 2, 2 * tiles - 1, 8, 128), jnp.int16),
            pltpu.VMEM((2, 4, tiles, 8, 128), jnp.int16),
            pltpu.VMEM((2, 4, tiles, 8, 128), jnp.int16),
            pltpu.VMEM((2, 6, tiles, 8, 128), jnp.int16),
            pltpu.VMEM((2, 6, tiles, 8, 128), jnp.int16),
            pltpu.VMEM((2, 128), jnp.float32),
            pltpu.VMEM((ny * nv - 1, 2, 128), jnp.float32),
            dma((7,)),
            dma((2, 2)),
            dma((2,)),
            dma((2,)),
            dma((2,)),
            dma((2, 2, 2)),
            dma,
            dma((2,)),
            dma,
            dma((2, 8)),
            dma,
            dma((2, 3, 2)),
            dma,
            dma((2, 3)),
            dma,
            dma((2, 4)),
            dma,
            dma((2, 6)),
            dma,
            dma,
        ],
        compiler_params=pltpu.CompilerParams(
            collective_id=0, has_side_effects=True, vmem_limit_bytes=55_500_000
        ),
    )(
        *(
            pltpu.with_memory_space_constraint(array, pltpu.HBM)
            for array in (occ_pairs, vir_pairs, amplitudes, hole_ints, occ_energy, vir_energy, ladder_ints)
        )
    )

    def hand_over(updated_ref, norm_ref, updated_out, norm_out, sem):
        copies = [
            pltpu.make_async_copy(src, dst, sem.at[n])
            for n, (src, dst) in enumerate(((updated_ref, updated_out), (norm_ref, norm_out)))
        ]
        for copy in copies:
            copy.start()
        for copy in copies:
            copy.wait()

    return pl.pallas_call(
        hand_over,
        out_shape=(
            jax.ShapeDtypeStruct(updated.shape, updated.dtype),
            jax.ShapeDtypeStruct(norm.shape, norm.dtype),
        ),
        in_specs=[vmem, vmem],
        out_specs=(pl.BlockSpec(memory_space=pl.ANY),) * 2,
        scratch_shapes=[dma((2,))],
        compiler_params=pltpu.CompilerParams(vmem_limit_bytes=2_000_000),
    )(updated, norm)


def solution(mesh):
    in_specs = (
        P("irrep", None, ("occ", "vir")),
        P("irrep", ("occ", "vir"), None),
        P("irrep", None, None),
        P("irrep", None),
        P("irrep", ("occ", "vir")),
        P(),
        P(),
    )
    out_specs = (P("irrep", None, ("occ", "vir")), P("irrep"))
    return jax.shard_map(body, mesh=mesh, in_specs=in_specs, out_specs=out_specs, check_vma=False)
```
